256 devices in a mesh: seq: 32 (over z, x), head: 8 (over y, core).
Axes of the slice: x: 4, y: 4, z: 8, core: 2. Of those that a mesh axis runs over, the one named last changes fastest.
Arguments:
- token_values: bfloat16 [8192, 5120], P('seq', 'head'), may hold values from -6 to 6
- gate_values: bfloat16 [8192, 5120], P('seq', 'head'), may hold values from -30 to 30
- state_in: bfloat16 [8192, 128], P('seq'), may hold values from -0.5 to 0.5
- state_out: bfloat16 [8192, 128], P('seq'), may hold values from -6 to 6
- step_size: float32 [8192, 80], P('seq', 'head'), may hold values from 0.02 to 0.2
- log_decay: float32 [8192, 80], P('seq', 'head'), may hold values from -1 to 0
- level_weight: bfloat16 [8192, 80, 14], P('seq', 'head'), may hold values from 0.25 to 2
- skip_weight: float32 [80], P('head'), may hold values from 0.5 to 1.5
- norm_gain: float32 [5120], P('head'), may hold values from 0.1 to 1.9
- out_weight: bfloat16 [5120, 2560], P('head'), may hold values from -0.078125 to 0.078125
Outputs:
- layer_out: bfloat16 [8192, 2560], P(('seq', 'head'))
The draws below stay inside these ranges and needn't reach their ends.
All inputs are finite; a program needn't handle non-finite values.
Results may differ from the reference program's by a relative error of at most 0.014.
Values may be sent and summed in bfloat16 or wider, within the bound.
No kernel may reach another device: no remote copies, remote signals or barrier semaphores. Data moves between devices by JAX's collectives and lax.ppermute only.
A program may use at most 64 MiB of HBM per device.

```python
import math
import jax
import jax.numpy as jnp
from jax import lax

DM = 2560
H = 80
P_SIZE = 64
N = 128
STRETCH_BITS = 6
STRETCH_DEV_BITS = 2
STRETCH = 64
TOK_DEV = 256
TOKENS = 8192
SEQ_BITS = 5
LEVELS = 14
N_HEAD = 8


def draw_log_decay(key, part):
    keys = jax.random.split(jax.random.fold_in(key, 101), 7)
    slow_share = 0.5
    slow = jax.random.uniform(keys[0], (H,)) < slow_share
    fast_rate = jnp.exp(jax.random.uniform(keys[1], (H,), minval=jnp.log(1.0 / (0.8 * STRETCH)), maxval=jnp.log(1.0 / (0.5 * STRETCH))))
    slow_rate = jnp.exp(jax.random.uniform(keys[2], (H,), minval=jnp.log(0.05), maxval=jnp.log(0.5))) / TOKENS
    fading_speed = jnp.where(slow, slow_rate, fast_rate)
    device_blocks = TOKENS // TOK_DEV
    fading_multiplier = jnp.exp(jax.random.uniform(keys[3], (device_blocks, H), minval=-0.7, maxval=0.7))
    fading_multiplier = jnp.repeat(fading_multiplier, TOK_DEV, axis=0)
    rough_guess = jnp.exp(jax.random.uniform(keys[4], (TOKENS, H), minval=jnp.log(0.5), maxval=jnp.log(1.5)))
    element_indices = jax.random.randint(keys[5], (2,), 0, TOKENS)
    blend_proportions = jax.random.uniform(keys[6], (2, H), minval=0.22, maxval=0.69)
    element_index = jnp.arange(TOKENS)[:, None]
    run_spans_count = jnp.where(element_index == element_indices[0], blend_proportions[0][None, :], 0.0) + jnp.where(element_index == element_indices[1], blend_proportions[1][None, :], 0.0)
    return jnp.clip(-(fading_speed[None, :] * fading_multiplier * rough_guess) - run_spans_count, -1.0, 0.0)


def draw_gate_values(key, part):
    keys = jax.random.split(jax.random.fold_in(key, 202), 3)
    rise = jnp.repeat(3.0 ** (jnp.arange(H, dtype=jnp.float32) / (H - 1)), P_SIZE)
    columns = rise * jnp.exp(jax.random.uniform(keys[0], (H * P_SIZE,), minval=0.0, maxval=jnp.log(3.3))) / 2.0
    scales = jnp.exp(jax.random.uniform(keys[1], (TOKENS,), minval=jnp.log(0.3), maxval=jnp.log(3.0)))
    base = jax.random.normal(keys[2], (TOKENS, H * P_SIZE))
    return jnp.clip(base * scales[:, None] * columns[None, :], -30.0, 30.0).astype(jnp.bfloat16)


def shard_levels(rng, extent, cuts, low, high):
    gain, own = 1.0, jax.random.fold_in(rng, 6)
    for axis_at, blocks in cuts:
        draws = jnp.exp(jax.random.uniform(jax.random.fold_in(own, axis_at), (blocks,), jnp.float32, low / len(cuts), high / len(cuts)))
        gain = gain * jnp.repeat(draws, extent[axis_at] // blocks).reshape([-1 if axis == axis_at else 1 for axis in range(len(extent))])
    return gain


def bell_draw(stream_key, extent, spread, reach, shards=(), kind=jnp.bfloat16):
    values = spread * jax.random.normal(stream_key, extent, jnp.float32)
    if shards:
        values = values * shard_levels(stream_key, extent, shards, -0.22, 0.18)
    return jnp.clip(values, -reach, reach).astype(kind)


def setup_inputs(seed: int = 0) -> dict:
    arg_keys = jax.random.split(jax.random.key(seed), 11)
    token_values = bell_draw(arg_keys[0], (TOKENS, H * P_SIZE), 1.0, 6.0, ((0, 32), (1, 8)))
    gate_values = draw_gate_values(jax.random.fold_in(arg_keys[10], 71), 0)
    state_in = bell_draw(arg_keys[2], (TOKENS, N), N ** -0.5, 0.5, ((0, 32),))
    state_out = bell_draw(arg_keys[3], (TOKENS, N), 1.0, 6.0, ((0, 32),))
    step_size = jnp.clip(jnp.exp(math.log(0.2) - 2.3025851 * jax.random.uniform(arg_keys[4], (TOKENS, H), jnp.float32) ** shard_levels(arg_keys[4], (TOKENS, H), ((0, 32), (1, 8)), -0.2, 0.2)), 0.02, 0.2)
    log_decay = draw_log_decay(jax.random.fold_in(arg_keys[10], 71), 0)
    level_weight = jnp.clip(jnp.exp(math.log(2.0) - 2.0794415 * jax.random.uniform(arg_keys[6], (TOKENS, H, LEVELS), jnp.float32) ** shard_levels(arg_keys[6], (TOKENS, H, LEVELS), ((0, 32), (1, 8)), -0.2, 0.2)), 0.25, 2.0).astype(jnp.bfloat16)
    skip_weight = jnp.clip(0.5 + 1.0 * jax.random.uniform(arg_keys[7], (H,), jnp.float32) ** shard_levels(arg_keys[7], (H,), ((0, 8),), -0.2, 0.2), 0.5, 1.5)
    norm_gain = jnp.clip(1.0 + 0.18 * jax.random.normal(arg_keys[8], (H * P_SIZE,), jnp.float32), 0.1, 1.9)
    out_weight = bell_draw(arg_keys[9], (H * P_SIZE, DM), (H * P_SIZE) ** -0.5, 0.078125, ((0, 8),))
    return {"token_values": token_values, "gate_values": gate_values, "state_in": state_in, "state_out": state_out, "step_size": step_size, "log_decay": log_decay, "level_weight": level_weight, "skip_weight": skip_weight, "norm_gain": norm_gain, "out_weight": out_weight}


EPSILON = 1e-05
HIGH = lax.Precision.HIGHEST

def bit_count(values, bit_width):
    counted = jnp.zeros(values.shape, jnp.int32)
    for shift in range(bit_width):
        counted = counted + (values >= 1 << shift).astype(jnp.int32)
    return counted

def stretch_levels():
    inside = jnp.arange(STRETCH, dtype=jnp.int32)
    later = inside[:, None]
    earlier = inside[None, :]
    causal = earlier <= later
    levels = bit_count(jnp.bitwise_xor(later, earlier), STRETCH_BITS)
    onehot = (levels[:, :, None] == jnp.arange(STRETCH_BITS + 1, dtype=jnp.int32)[None, None, :]) & causal[:, :, None]
    return (causal, onehot.astype(jnp.float32))

def head_mix(scores, query_rows, key_rows, causal, onehot, packed):
    values, steps, decays, weights, skip = packed
    blocks_all = TOKENS // STRETCH
    inputs = (values * steps[:, None]).reshape(blocks_all, STRETCH, P_SIZE)
    within = jnp.cumsum(decays.reshape(blocks_all, STRETCH), axis=1)
    totals = within[:, -1]
    weights = weights.reshape(blocks_all, STRETCH, LEVELS)
    gaps = jnp.where(causal[None], within[:, :, None] - within[:, None, :], -jnp.inf)
    mixing = jnp.einsum('ctl,tsl->cts', weights[:, :, :STRETCH_BITS + 1], onehot) * jnp.exp(gaps) * scores
    output = jnp.einsum('cts,csp->ctp', mixing, inputs, precision=HIGH)
    to_end = jnp.exp(totals[:, None] - within)
    states = jnp.einsum('csn,csp->cnp', key_rows * to_end[:, :, None], inputs, precision=HIGH)
    queries = query_rows * jnp.exp(within)[:, :, None]
    block_ids = jnp.arange(blocks_all, dtype=jnp.int32)
    blocks = states
    block_totals = totals
    for depth in range(1, STRETCH_DEV_BITS + SEQ_BITS + 1):
        size = 2 ** (depth - 1)
        grouped = totals.reshape(blocks_all // size, size)
        before = (jnp.cumsum(grouped, axis=1) - grouped).reshape(blocks_all)
        upper = (block_ids >> depth - 1 & 1).astype(jnp.float32)
        sibling = jnp.bitwise_xor(block_ids >> depth - 1, 1).astype(jnp.int32)
        carried = blocks[sibling] * (upper * jnp.exp(before))[:, None, None]
        reached = jnp.einsum('ctn,cnp->ctp', queries, carried, precision=HIGH)
        output = output + weights[:, :, STRETCH_BITS + depth, None] * reached
        paired = blocks.reshape(-1, 2, N, P_SIZE)
        pair_totals = block_totals.reshape(-1, 2)
        blocks = jnp.exp(pair_totals[:, 1])[:, None, None] * paired[:, 0] + paired[:, 1]
        block_totals = pair_totals[:, 0] + pair_totals[:, 1]
    return output.reshape(TOKENS, P_SIZE) + skip * values

def reference(token_values, gate_values, state_in, state_out, step_size, log_decay, level_weight, skip_weight, norm_gain, out_weight):
    blocks_all = TOKENS // STRETCH
    causal, onehot = stretch_levels()
    query_rows = state_out.astype(jnp.float32).reshape(blocks_all, STRETCH, N)
    key_rows = state_in.astype(jnp.float32).reshape(blocks_all, STRETCH, N)
    scores = jnp.einsum('ctn,csn->cts', query_rows, key_rows)
    values_heads = jnp.transpose(token_values.astype(jnp.float32).reshape(TOKENS, H, P_SIZE), (1, 0, 2))
    steps_heads = jnp.transpose(step_size)
    decays_heads = jnp.transpose(log_decay)
    weights_heads = jnp.transpose(level_weight.astype(jnp.float32), (1, 0, 2))

    def per_head(packed):
        return head_mix(scores, query_rows, key_rows, causal, onehot, packed)
    mixed_heads = lax.map(per_head, (values_heads, steps_heads, decays_heads, weights_heads, skip_weight))
    mixed = jnp.transpose(mixed_heads, (1, 0, 2)).reshape(TOKENS, H * P_SIZE)
    gated = mixed * jax.nn.silu(gate_values.astype(jnp.float32))
    square = lax.optimization_barrier(jnp.mean(gated * gated, axis=1, keepdims=True))
    features = (gated * lax.rsqrt(square + EPSILON) * norm_gain).astype(jnp.bfloat16)
    width = H * P_SIZE // N_HEAD

    def add_group(total, group):
        picked = lax.dynamic_slice_in_dim(features, group * width, width, 1)
        rows_w = lax.dynamic_slice_in_dim(out_weight, group * width, width, 0)
        partial_value = jnp.dot(picked, rows_w, preferred_element_type=jnp.float32).astype(jnp.bfloat16)
        return (total + partial_value.astype(jnp.float32), None)
    summed, _ = lax.scan(add_group, jnp.zeros((TOKENS, DM), jnp.float32), jnp.arange(N_HEAD, dtype=jnp.int32))
    return summed.astype(jnp.bfloat16)
```

```python
import jax
import jax.numpy as jnp
from jax import lax
from jax.experimental import pallas as pl
from jax.experimental.pallas import tpu as pltpu
from jax.sharding import PartitionSpec as P

H = 80
HEADS = 10
P_SIZE = 64
N = 128
TOK = 256
WIDTH = HEADS * P_SIZE
DM = 2560
WIDE = DM + 128
LOCAL_LEVELS = 9
PAY = WIDTH + 32

EPSILON = 1e-05

F32 = jnp.float32
BF16 = jnp.bfloat16


def dot(a, b):
    return jnp.dot(a, b, preferred_element_type=F32)


def split_two(value):
    high = value.astype(BF16)
    return high, (value - high.astype(F32)).astype(BF16)


def pad_heads(value):
    return jnp.concatenate([value, jnp.zeros((16 - HEADS, value.shape[1]), F32)], axis=0)


def state_kernel(x_ref, k_ref, step_ref, decay_ref, pay_ref, state_ref, xt_ref, cum_ref, tot_ref):
    decay = pad_heads(decay_ref[...])
    step = pad_heads(step_ref[...])
    high = decay.astype(BF16)
    rest = decay - high.astype(F32)
    mid, low = split_two(rest)
    earlier = lax.broadcasted_iota(jnp.int32, (TOK, TOK), 0)
    later = lax.broadcasted_iota(jnp.int32, (TOK, TOK), 1)
    upto = jnp.where(earlier <= later, 1.0, 0.0).astype(BF16)
    parts = dot(jnp.concatenate([high, mid, low], axis=0), upto)
    cum = parts[0:16] + parts[16:32] + parts[32:48]
    total = jnp.broadcast_to(cum[:, TOK - 1 : TOK], (16, 128))
    cum_ref[...] = cum
    tot_ref[...] = total
    high, low = split_two(total)
    pay_ref[WIDTH : WIDTH + 16, :] = high
    pay_ref[WIDTH + 16 : WIDTH + 32, :] = low
    coef = step * jnp.exp(cum[:, TOK - 1 : TOK] - cum)
    keys = k_ref[...]
    for j in range(WIDTH // 128):
        rows = slice(j * 128, (j + 1) * 128)
        xt = x_ref[:, rows].astype(F32).T
        xt_ref[rows, :] = xt.astype(BF16)
        scaled = jnp.concatenate(
            [xt[0:64] * coef[2 * j : 2 * j + 1], xt[64:128] * coef[2 * j + 1 : 2 * j + 2]], axis=0
        )
        state = dot(scaled.astype(BF16), keys)
        state_ref[rows, :] = state
        pay_ref[rows, :] = state.astype(BF16)


def local_kernel(xt_ref, k_ref, q_ref, step_ref, cum_ref, w_ref, skip_ref, out_ref, qt_ref):
    qt = q_ref[...].astype(F32).T.astype(BF16)
    qt_ref[...] = qt
    scores = dot(k_ref[...], qt)
    cum = cum_ref[...]
    cols = cum.T
    early = lax.broadcasted_iota(jnp.int32, (128, 128), 0)
    late = lax.broadcasted_iota(jnp.int32, (128, 128), 1)
    differ = jnp.bitwise_xor(early, late)
    level = jnp.zeros((128, 128), jnp.int32)
    for shift in range(7):
        level = level + (differ >= 1 << shift).astype(jnp.int32)
    level = jnp.where(early <= late, level, -1)
    for h in range(HEADS):
        weights = w_ref[h, 0:LOCAL_LEVELS, :].astype(F32)
        xt = xt_ref[h * 64 : (h + 1) * 64, :].astype(F32)
        inputs = (xt * step_ref[h : h + 1, :]).astype(BF16)

        def faded(i, j):
            s, t = slice(i * 128, (i + 1) * 128), slice(j * 128, (j + 1) * 128)
            gap = jnp.minimum(cum[h : h + 1, t] - cols[s, h : h + 1], 0.0)
            return jnp.exp(gap) * scores[s, t]

        def diagonal(i):
            t = slice(i * 128, (i + 1) * 128)
            picked = jnp.zeros((128, 128), F32)
            for l in range(LOCAL_LEVELS - 1):
                picked = jnp.where(level == l, weights[l : l + 1, t], picked)
            return (faded(i, i) * picked).astype(BF16)

        first = diagonal(0)
        second = jnp.concatenate(
            [(faded(0, 1) * weights[8:9, 128:256]).astype(BF16), diagonal(1)], axis=0
        )
        mixed = jnp.concatenate([dot(inputs[:, 0:128], first), dot(inputs, second)], axis=1)
        out_ref[h * 64 : (h + 1) * 64, :] = mixed + skip_ref[h] * xt


def combine_kernel(bit, state_ref, tot_ref, span_ref, recv_ref, pay_ref, new_ref, ntot_ref, nspan_ref):
    upper = ((lax.axis_index("seq") >> bit) & 1) > 0
    total = tot_ref[...]
    other = recv_ref[WIDTH : WIDTH + 16, :].astype(F32) + recv_ref[WIDTH + 16 : WIDTH + 32, :].astype(F32)
    new_total = total + other
    ntot_ref[...] = new_total
    nspan_ref[...] = span_ref[...] + jnp.where(upper, other, 0.0)
    high, low = split_two(new_total)
    pay_ref[WIDTH : WIDTH + 16, :] = high
    pay_ref[WIDTH + 16 : WIDTH + 32, :] = low
    for_other = jnp.where(upper, jnp.exp(total), 1.0)
    for_mine = jnp.where(upper, 1.0, jnp.exp(other))
    for h in range(HEADS):
        rows = slice(h * 64, (h + 1) * 64)
        new = for_other[h : h + 1] * recv_ref[rows, :].astype(F32) + for_mine[h : h + 1] * state_ref[rows, :]
        new_ref[rows, :] = new
        pay_ref[rows, :] = new.astype(BF16)


def far_term(recv_ref, qt, h, coef):
    rows = slice(h * 64, (h + 1) * 64)
    return dot(recv_ref[rows, :], qt) * coef


def far_coef(bit, cum, span_ref, w_ref, h):
    upper = ((lax.axis_index("seq") >> bit) & 1) > 0
    lift = jnp.exp(cum[h : h + 1, :] + span_ref[h : h + 1, 0:1])
    weight = w_ref[h, LOCAL_LEVELS + bit : LOCAL_LEVELS + bit + 1, :].astype(F32)
    return jnp.where(upper, lift * weight, 0.0)


def near_kernel(local_ref, r0, r1, r2, r3, s0, s1, s2, s3, qt_ref, cum_ref, w_ref, out_ref):
    qt = qt_ref[...]
    cum = cum_ref[...]
    for h in range(HEADS):
        rows = slice(h * 64, (h + 1) * 64)
        total = local_ref[rows, :]
        for bit, (recv, span) in enumerate(((r0, s0), (r1, s1), (r2, s2), (r3, s3))):
            total = total + far_term(recv, qt, h, far_coef(bit, cum, span, w_ref, h))
        out_ref[rows, :] = total


def project_kernel(
    near_ref, recv_ref, span_ref, qt_ref, cum_ref, w_ref, gate_ref, gain_ref, ow_ref,
    mine_ref, theirs_ref, feat_ref, square_ref,
):
    qt = qt_ref[...]
    cum = cum_ref[...]
    squares = jnp.zeros((TOK, 1), F32)
    for j in range(WIDTH // 128):
        cols = slice(j * 128, (j + 1) * 128)
        far = jnp.concatenate(
            [far_term(recv_ref, qt, h, far_coef(4, cum, span_ref, w_ref, h)) for h in (2 * j, 2 * j + 1)],
            axis=0,
        )
        mixed = (near_ref[cols, :] + far).T
        gate = gate_ref[:, cols].astype(F32)
        gated = mixed * (gate / (1.0 + jnp.exp(-gate)))
        squares = squares + jnp.sum(gated * gated, axis=1, keepdims=True)
        feat_ref[:, cols] = (gated * gain_ref[:, cols]).astype(BF16)
    square_ref[...] = jnp.broadcast_to(squares, (TOK, 128))
    core = lax.axis_index("head") & 1
    lane = lax.broadcasted_iota(jnp.int32, (32, 128), 1)
    for out_ref, side in ((theirs_ref, 1 - core), (mine_ref, core)):
        starts = [pl.multiple_of((2 * y + side) * 32, 32) for y in range(4)]
        rows = jnp.concatenate([feat_ref[pl.ds(s, 32), :] for s in starts], axis=0)
        out_ref[:, 0:DM] = dot(rows, ow_ref[...]).astype(BF16)
        for y, s in enumerate(starts):
            high, low = split_two(square_ref[pl.ds(s, 32), :])
            out_ref[y * 32 : (y + 1) * 32, DM:WIDE] = jnp.where(
                lane < 64, high.astype(F32), low.astype(F32)
            ).astype(BF16)


def squares_of(ref, rows):
    return ref[rows, DM : DM + 1].astype(F32) + ref[rows, DM + 64 : DM + 65].astype(F32)


def pair_kernel(mine_ref, recv_ref, own_ref, o1, o2, o3):
    y = lax.axis_index("head") >> 1
    lane = lax.broadcasted_iota(jnp.int32, (32, 128), 1)
    for k, out_ref in enumerate((own_ref, o1, o2, o3)):
        rows = pl.ds(pl.multiple_of(jnp.bitwise_xor(y, k) * 32, 32), 32)
        total = mine_ref[rows, 0:DM].astype(F32) + recv_ref[rows, 0:DM].astype(F32)
        out_ref[:, 0:DM] = total.astype(out_ref.dtype)
        square = jnp.broadcast_to(squares_of(mine_ref, rows) + squares_of(recv_ref, rows), (32, 128))
        high, low = split_two(square)
        out_ref[:, DM:WIDE] = jnp.where(lane < 64, high.astype(F32), low.astype(F32)).astype(out_ref.dtype)


def final_kernel(own_ref, r1, r2, r3, out_ref):
    every = slice(0, 32)
    square = squares_of(own_ref, every) + squares_of(r1, every) + squares_of(r2, every) + squares_of(r3, every)
    scale = lax.rsqrt(square * (1.0 / (H * P_SIZE)) + EPSILON)
    total = own_ref[:, 0:DM].astype(F32)
    for ref in (r1, r2, r3):
        total = total + ref[:, 0:DM].astype(F32)
    out_ref[...] = (total * scale).astype(BF16)


def call(kernel, outs, *args, scratch=(), flops=0, name=None, smem=()):
    specs = [
        pl.BlockSpec(memory_space=pltpu.SMEM if i in smem else pltpu.VMEM) for i in range(len(args))
    ]
    shapes = [jax.ShapeDtypeStruct(shape, dtype) for shape, dtype in outs]
    outputs = pl.pallas_call(
        kernel,
        out_shape=shapes,
        in_specs=specs,
        out_specs=[pl.BlockSpec(memory_space=pltpu.VMEM) for _ in outs],
        scratch_shapes=list(scratch),
        compiler_params=pltpu.CompilerParams(vmem_limit_bytes=48 << 20),
        cost_estimate=pl.CostEstimate(flops=flops, transcendentals=0, bytes_accessed=flops // 100),
        name=name,
    )(*args)
    return outputs


SENDS = (
    [(d, d ^ 1) for d in range(32)],
    [(d, d ^ 3) for d in range(32)],
    [(d, d ^ 4) for d in range(32)],
    [(d, d ^ 8) for d in range(32)],
    [(d, d ^ 28) for d in range(16)],
)


def on_device(token_values, gate_values, state_in, state_out, step_size, log_decay, level_weight, skip_weight, norm_gain, out_weight):
    step = jnp.transpose(step_size)
    decay = jnp.transpose(log_decay)
    weight = jnp.transpose(level_weight, (1, 2, 0))
    pay, state, xt, cum, total = call(
        state_kernel,
        [((PAY, N), BF16), ((WIDTH, N), F32), ((WIDTH, TOK), BF16), ((16, TOK), F32), ((16, 128), F32)],
        token_values, state_in, step, decay, flops=10**8, name="state",
    )
    local, qt = call(
        local_kernel,
        [((WIDTH, TOK), F32), ((N, TOK), BF16)],
        xt, state_in, state_out, step, cum, weight, skip_weight,
        flops=5 * 10**9, name="local", smem=(6,),
    )
    span = jnp.zeros((16, 128), F32)
    recvs, spans = [], []
    for bit in range(5):
        recv = lax.ppermute(pay, "seq", SENDS[bit])
        recvs.append(recv)
        spans.append(span)
        if bit < 4:
            pay, state, total, span = call(
                lambda *refs, bit=bit: combine_kernel(bit, *refs),
                [((PAY, N), BF16), ((WIDTH, N), F32), ((16, 128), F32), ((16, 128), F32)],
                state, total, span, recv, flops=10**6, name="combine",
            )
    (near,) = call(
        near_kernel, [((WIDTH, TOK), F32)], local, *recvs[:4], *spans[:4], qt, cum, weight,
        flops=2 * 10**9, name="near",
    )
    mine, theirs = call(
        project_kernel,
        [((128, WIDE), BF16), ((128, WIDE), BF16)],
        near, recvs[4], spans[4], qt, cum, weight, gate_values, norm_gain[None, :], out_weight,
        scratch=[pltpu.VMEM((TOK, WIDTH), BF16), pltpu.VMEM((TOK, 128), F32)],
        flops=10**9, name="project",
    )
    recv = lax.ppermute(theirs, "head", [(g, g ^ 1) for g in range(8)])
    own, *sends = call(
        pair_kernel,
        [((32, WIDE), F32)] + [((32, WIDE), BF16)] * 3,
        mine, recv, flops=10**6, name="pair",
    )
    got = [lax.ppermute(sends[k - 1], "head", [(g, g ^ (2 * k)) for g in range(8)]) for k in (1, 2, 3)]
    (out,) = call(final_kernel, [((32, DM), BF16)], own, *got, flops=10**6, name="final")
    return out


def solution(mesh):
    placed = (
        P("seq", "head"),
        P("seq", "head"),
        P("seq", None),
        P("seq", None),
        P("seq", "head"),
        P("seq", "head"),
        P("seq", "head", None),
        P("head"),
        P("head"),
        P("head", None),
    )
    return jax.shard_map(
        on_device, mesh=mesh, in_specs=placed, out_specs=P(("seq", "head"), None), check_vma=False
    )
```

```python
import jax
import jax.numpy as jnp
from jax import lax
from jax.experimental import pallas as pl
from jax.experimental.pallas import tpu as pltpu
from jax.sharding import PartitionSpec as P

H = 80
HEADS = 10
P_SIZE = 64
N = 128
TOK = 256
WIDTH = HEADS * P_SIZE
DM = 2560
WIDE = DM + 128
LOCAL_LEVELS = 9
PAY = WIDTH + 32

EPSILON = 1e-05

F32 = jnp.float32
BF16 = jnp.bfloat16


def dot(a, b):
    return jnp.dot(a, b, preferred_element_type=F32)


def split_two(value):
    high = value.astype(BF16)
    return high, (value - high.astype(F32)).astype(BF16)


def pad_heads(value):
    return jnp.concatenate([value, jnp.zeros((16 - HEADS, value.shape[1]), F32)], axis=0)


def fetch(sources, targets, sems):
    copies = [pltpu.make_async_copy(s, t, sems.at[i]) for i, (s, t) in enumerate(zip(sources, targets))]
    for copy in copies:
        copy.start()
    return copies


def state_kernel(
    x_in, k_in, step_in, decay_in, pay_ref, state_ref, xt_ref, cum_ref, tot_ref,
    x_ref, k_ref, step_ref, decay_ref, sems,
):
    copies = fetch((decay_in, step_in, k_in, x_in), (decay_ref, step_ref, k_ref, x_ref), sems)
    copies[0].wait()
    copies[1].wait()
    decay = pad_heads(decay_ref[...])
    step = pad_heads(step_ref[...])
    high = decay.astype(BF16)
    rest = decay - high.astype(F32)
    mid, low = split_two(rest)
    earlier = lax.broadcasted_iota(jnp.int32, (TOK, TOK), 0)
    later = lax.broadcasted_iota(jnp.int32, (TOK, TOK), 1)
    upto = jnp.where(earlier <= later, 1.0, 0.0).astype(BF16)
    parts = dot(jnp.concatenate([high, mid, low], axis=0), upto)
    cum = parts[0:16] + parts[16:32] + parts[32:48]
    total = jnp.broadcast_to(cum[:, TOK - 1 : TOK], (16, 128))
    cum_ref[...] = cum
    tot_ref[...] = total
    high, low = split_two(total)
    pay_ref[WIDTH : WIDTH + 16, :] = high
    pay_ref[WIDTH + 16 : WIDTH + 32, :] = low
    coef = step * jnp.exp(cum[:, TOK - 1 : TOK] - cum)
    copies[2].wait()
    copies[3].wait()
    keys = k_ref[...]
    for j in range(WIDTH // 128):
        rows = slice(j * 128, (j + 1) * 128)
        xt = x_ref[:, rows].astype(F32).T
        xt_ref[rows, :] = xt.astype(BF16)
        scaled = jnp.concatenate(
            [xt[0:64] * coef[2 * j : 2 * j + 1], xt[64:128] * coef[2 * j + 1 : 2 * j + 2]], axis=0
        )
        state = dot(scaled.astype(BF16), keys)
        state_ref[rows, :] = state
        pay_ref[rows, :] = state.astype(BF16)


def local_kernel(
    xt_ref, cum_ref, skip_ref, k_in, q_in, step_in, w_in, out_ref, qt_ref,
    k_ref, q_ref, step_ref, w_ref, sems,
):
    copies = fetch((q_in, k_in, step_in, w_in), (q_ref, k_ref, step_ref, w_ref), sems)
    copies[0].wait()
    copies[1].wait()
    qt = q_ref[...].astype(F32).T.astype(BF16)
    qt_ref[...] = qt
    scores = dot(k_ref[...], qt)
    cum = cum_ref[...]
    cols = cum.T
    early = lax.broadcasted_iota(jnp.int32, (128, 128), 0)
    late = lax.broadcasted_iota(jnp.int32, (128, 128), 1)
    differ = jnp.bitwise_xor(early, late)
    level = jnp.zeros((128, 128), jnp.int32)
    for shift in range(7):
        level = level + (differ >= 1 << shift).astype(jnp.int32)
    level = jnp.where(early <= late, level, -1)
    copies[2].wait()
    copies[3].wait()
    for h in range(HEADS):
        weights = w_ref[h, 0:LOCAL_LEVELS, :].astype(F32)
        xt = xt_ref[h * 64 : (h + 1) * 64, :].astype(F32)
        inputs = (xt * step_ref[h : h + 1, :]).astype(BF16)

        def faded(i, j):
            s, t = slice(i * 128, (i + 1) * 128), slice(j * 128, (j + 1) * 128)
            gap = jnp.minimum(cum[h : h + 1, t] - cols[s, h : h + 1], 0.0)
            return jnp.exp(gap) * scores[s, t]

        def diagonal(i):
            t = slice(i * 128, (i + 1) * 128)
            picked = jnp.zeros((128, 128), F32)
            for l in range(LOCAL_LEVELS - 1):
                picked = jnp.where(level == l, weights[l : l + 1, t], picked)
            return (faded(i, i) * picked).astype(BF16)

        first = diagonal(0)
        second = jnp.concatenate(
            [(faded(0, 1) * weights[8:9, 128:256]).astype(BF16), diagonal(1)], axis=0
        )
        mixed = jnp.concatenate([dot(inputs[:, 0:128], first), dot(inputs, second)], axis=1)
        out_ref[h * 64 : (h + 1) * 64, :] = mixed + skip_ref[h] * xt


def combine_kernel(bit, state_ref, tot_ref, span_ref, recv_ref, pay_ref, new_ref, ntot_ref, nspan_ref):
    upper = ((lax.axis_index("seq") >> bit) & 1) > 0
    total = tot_ref[...]
    other = recv_ref[WIDTH : WIDTH + 16, :].astype(F32) + recv_ref[WIDTH + 16 : WIDTH + 32, :].astype(F32)
    new_total = total + other
    ntot_ref[...] = new_total
    nspan_ref[...] = span_ref[...] + jnp.where(upper, other, 0.0)
    high, low = split_two(new_total)
    pay_ref[WIDTH : WIDTH + 16, :] = high
    pay_ref[WIDTH + 16 : WIDTH + 32, :] = low
    for_other = jnp.where(upper, jnp.exp(total), 1.0)
    for_mine = jnp.where(upper, 1.0, jnp.exp(other))
    for h in range(HEADS):
        rows = slice(h * 64, (h + 1) * 64)
        new = for_other[h : h + 1] * recv_ref[rows, :].astype(F32) + for_mine[h : h + 1] * state_ref[rows, :]
        new_ref[rows, :] = new
        pay_ref[rows, :] = new.astype(BF16)


def totals_of(recv_ref):
    return recv_ref[WIDTH : WIDTH + 16, :].astype(F32) + recv_ref[WIDTH + 16 : WIDTH + 32, :].astype(F32)


def quad_kernel(_, r3, r2, r1, state_ref, tot_ref, pay_ref, pair_ref, new_ref, ntot_ref, span1_ref, span2_ref):
    x = lax.axis_index("seq")
    odd, upper = (x & 1) > 0, (x & 2) > 0
    t0 = tot_ref[...]
    t1, t2, t3 = totals_of(r1), totals_of(r2), totals_of(r3)
    total = t0 + t1 + t2 + t3
    ntot_ref[...] = total
    high, low = split_two(total)
    pay_ref[WIDTH : WIDTH + 16, :] = high
    pay_ref[WIDTH + 16 : WIDTH + 32, :] = low
    span1 = jnp.where(odd, t1, 0.0)
    span1_ref[...] = span1
    span2_ref[...] = span1 + jnp.where(upper, t2 + t3, 0.0)
    mine_to = jnp.where(odd, 0.0, t1)
    next_to = jnp.where(odd, t0, 0.0)
    across_to = jnp.where(odd, 0.0, t3)
    far_to = jnp.where(odd, t2, 0.0)
    lower_pair = jnp.exp(jnp.where(upper, t0 + t1, 0.0))
    f2, f3 = jnp.exp(across_to), jnp.exp(far_to)
    other = jnp.where(upper, 0.0, t2 + t3)
    f0, f1 = jnp.exp(mine_to + other), jnp.exp(next_to + other)
    for h in range(HEADS):
        rows = slice(h * 64, (h + 1) * 64)
        row = slice(h, h + 1)
        pair = f2[row] * r2[rows, :].astype(F32) + f3[row] * r3[rows, :].astype(F32)
        pair_ref[rows, :] = pair.astype(BF16)
        new = f0[row] * state_ref[rows, :] + f1[row] * r1[rows, :].astype(F32) + lower_pair[row] * pair
        new_ref[rows, :] = new
        pay_ref[rows, :] = new.astype(BF16)


def last_combine_kernel(state_ref, tot_ref, span_ref, recv_ref, pay_ref, nspan_ref):
    upper = ((lax.axis_index("seq") >> 3) & 1) > 0
    total = tot_ref[...]
    other = recv_ref[WIDTH : WIDTH + 16, :].astype(F32) + recv_ref[WIDTH + 16 : WIDTH + 32, :].astype(F32)
    nspan_ref[...] = span_ref[...] + jnp.where(upper, other, 0.0)
    for_other = jnp.where(upper, jnp.exp(total), 1.0)
    for_mine = jnp.where(upper, 1.0, jnp.exp(other))
    for h in range(HEADS):
        rows = slice(h * 64, (h + 1) * 64)
        new = for_other[h : h + 1] * recv_ref[rows, :].astype(F32) + for_mine[h : h + 1] * state_ref[rows, :]
        pay_ref[rows, :] = new.astype(BF16)


def far_term(recv_ref, qt, h, coef):
    rows = slice(h * 64, (h + 1) * 64)
    return dot(recv_ref[rows, :], qt) * coef


def far_coef(bit, cum, span_ref, w_ref, h):
    upper = ((lax.axis_index("seq") >> bit) & 1) > 0
    lift = jnp.exp(cum[h : h + 1, :] + span_ref[h : h + 1, 0:1])
    weight = w_ref[h, LOCAL_LEVELS + bit : LOCAL_LEVELS + bit + 1, :].astype(F32)
    return jnp.where(upper, lift * weight, 0.0)


def near_kernel(local_ref, r0, r1, r2, r3, s0, s1, s2, s3, qt_ref, cum_ref, w_ref, out_ref):
    qt = qt_ref[...]
    cum = cum_ref[...]
    for h in range(HEADS):
        rows = slice(h * 64, (h + 1) * 64)
        total = local_ref[rows, :]
        for bit, (recv, span) in enumerate(((r0, s0), (r1, s1), (r2, s2), (r3, s3))):
            total = total + far_term(recv, qt, h, far_coef(bit, cum, span, w_ref, h))
        out_ref[rows, :] = total


def project_kernel(
    near_ref, recv_ref, span_ref, qt_ref, cum_ref, w_ref, gate_ref, gain_ref, ow_ref,
    theirs_ref, feat_ref, square_ref,
):
    qt = qt_ref[...]
    cum = cum_ref[...]
    squares = jnp.zeros((TOK, 1), F32)
    for j in range(WIDTH // 128):
        cols = slice(j * 128, (j + 1) * 128)
        far = jnp.concatenate(
            [far_term(recv_ref, qt, h, far_coef(4, cum, span_ref, w_ref, h)) for h in (2 * j, 2 * j + 1)],
            axis=0,
        )
        mixed = (near_ref[cols, :] + far).T
        gate = gate_ref[:, cols].astype(F32)
        gated = mixed * (gate / (1.0 + jnp.exp(-gate)))
        squares = squares + jnp.sum(gated * gated, axis=1, keepdims=True)
        feat_ref[:, cols] = (gated * gain_ref[:, cols]).astype(BF16)
    square_ref[...] = jnp.broadcast_to(squares, (TOK, 128))
    product_rows(feat_ref, square_ref, ow_ref, theirs_ref, 1 - (lax.axis_index("head") & 1))


def product_rows(feat_ref, square_ref, ow_ref, out_ref, side):
    lane = lax.broadcasted_iota(jnp.int32, (32, 128), 1)
    starts = [pl.multiple_of((2 * y + side) * 32, 32) for y in range(4)]
    rows = jnp.concatenate([feat_ref[pl.ds(s, 32), :] for s in starts], axis=0)
    out_ref[:, 0:DM] = dot(rows, ow_ref[...]).astype(BF16)
    for y, s in enumerate(starts):
        high, low = split_two(square_ref[pl.ds(s, 32), :])
        out_ref[y * 32 : (y + 1) * 32, DM:WIDE] = jnp.where(
            lane < 64, high.astype(F32), low.astype(F32)
        ).astype(BF16)


def own_rows_kernel(feat_ref, square_ref, ow_ref, mine_ref):
    product_rows(feat_ref, square_ref, ow_ref, mine_ref, lax.axis_index("head") & 1)


def squares_of(ref, rows):
    return ref[rows, DM : DM + 1].astype(F32) + ref[rows, DM + 64 : DM + 65].astype(F32)


def pair_kernel(mine_ref, recv_ref, own_ref, o1, o2, o3):
    y = lax.axis_index("head") >> 1
    lane = lax.broadcasted_iota(jnp.int32, (32, 128), 1)
    for k, out_ref in enumerate((own_ref, o1, o2, o3)):
        rows = pl.ds(pl.multiple_of(jnp.bitwise_xor(y, k) * 32, 32), 32)
        total = mine_ref[rows, 0:DM].astype(F32) + recv_ref[rows, 0:DM].astype(F32)
        out_ref[:, 0:DM] = total.astype(out_ref.dtype)
        square = jnp.broadcast_to(squares_of(mine_ref, rows) + squares_of(recv_ref, rows), (32, 128))
        high, low = split_two(square)
        out_ref[:, DM:WIDE] = jnp.where(lane < 64, high.astype(F32), low.astype(F32)).astype(out_ref.dtype)


def final_kernel(own_ref, r1, r2, r3, out_ref):
    every = slice(0, 32)
    square = squares_of(own_ref, every) + squares_of(r1, every) + squares_of(r2, every) + squares_of(r3, every)
    scale = lax.rsqrt(square * (1.0 / (H * P_SIZE)) + EPSILON)
    total = own_ref[:, 0:DM].astype(F32)
    for ref in (r1, r2, r3):
        total = total + ref[:, 0:DM].astype(F32)
    out_ref[...] = (total * scale).astype(BF16)


def call(kernel, outs, *args, scratch=(), flops=0, name=None, smem=(), hbm=(), free=()):
    def space(i):
        if i in smem:
            return pltpu.SMEM
        if i in hbm:
            return pltpu.HBM
        return pl.ANY if i in free else pltpu.VMEM

    specs = [pl.BlockSpec(memory_space=space(i)) for i in range(len(args))]
    args = [pltpu.with_memory_space_constraint(a, pltpu.HBM) if i in hbm else a for i, a in enumerate(args)]
    shapes = [jax.ShapeDtypeStruct(shape, dtype) for shape, dtype in outs]
    outputs = pl.pallas_call(
        kernel,
        out_shape=shapes,
        in_specs=specs,
        out_specs=[pl.BlockSpec(memory_space=pltpu.VMEM) for _ in outs],
        scratch_shapes=list(scratch),
        compiler_params=pltpu.CompilerParams(vmem_limit_bytes=48 << 20),
        cost_estimate=pl.CostEstimate(flops=flops, transcendentals=0, bytes_accessed=flops // 100),
        name=name,
    )(*args)
    return outputs


def on_device(token_values, gate_values, state_in, state_out, step_size, log_decay, level_weight, skip_weight, norm_gain, out_weight):
    step = jnp.transpose(step_size)
    decay = jnp.transpose(log_decay)
    weight = jnp.transpose(level_weight, (1, 2, 0))
    pay, state, xt, cum, total = call(
        state_kernel,
        [((PAY, N), BF16), ((WIDTH, N), F32), ((WIDTH, TOK), BF16), ((16, TOK), F32), ((16, 128), F32)],
        token_values, state_in, step, decay, flops=10**8, name="state", hbm=(0, 1, 2, 3),
        scratch=[
            pltpu.VMEM((TOK, WIDTH), BF16), pltpu.VMEM((TOK, N), BF16), pltpu.VMEM((HEADS, TOK), F32),
            pltpu.VMEM((HEADS, TOK), F32), pltpu.SemaphoreType.DMA((4,)),
        ],
    )
    local, qt = call(
        local_kernel,
        [((WIDTH, TOK), F32), ((N, TOK), BF16)],
        xt, cum, skip_weight, state_in, state_out, step, weight,
        flops=5 * 10**9, name="local", smem=(2,), hbm=(3, 4, 5, 6),
        scratch=[
            pltpu.VMEM((TOK, N), BF16), pltpu.VMEM((TOK, N), BF16), pltpu.VMEM((HEADS, TOK), F32),
            pltpu.VMEM((HEADS, 14, TOK), BF16), pltpu.SemaphoreType.DMA((4,)),
        ],
    )
    r3, r2, r1 = [lax.ppermute(pay, "seq", [(d, d ^ k) for d in range(32)]) for k in (3, 2, 1)]
    pay, pair, state, total, span1, span2 = call(
        quad_kernel,
        [((PAY, N), BF16), ((WIDTH, N), BF16), ((WIDTH, N), F32)] + [((16, 128), F32)] * 3,
        local, r3, r2, r1, state, total, flops=10**6, name="quad", free=(0,),
    )
    recvs, spans = [r1, pair], [jnp.zeros((16, 128), F32), span1, span2]
    recvs.append(lax.ppermute(pay, "seq", [(d, d ^ 4) for d in range(32)]))
    pay, state, total, span = call(
        lambda *refs: combine_kernel(2, *refs),
        [((PAY, N), BF16), ((WIDTH, N), F32), ((16, 128), F32), ((16, 128), F32)],
        state, total, span2, recvs[2], flops=10**6, name="combine",
    )
    spans.append(span)
    recvs.append(lax.ppermute(pay, "seq", [(d, d ^ 12) for d in range(32)]))
    pay, span = call(
        last_combine_kernel, [((WIDTH, N), BF16), ((16, 128), F32)],
        state, total, span, recvs[3], flops=10**6, name="combine",
    )
    spans.append(span)
    recvs.append(lax.ppermute(pay, "seq", [(d, d ^ 28) for d in range(32)]))
    (near,) = call(
        near_kernel, [((WIDTH, TOK), F32)], local, *recvs[:4], *spans[:4], qt, cum, weight,
        flops=2 * 10**9, name="near",
    )
    theirs, feat, square = call(
        project_kernel,
        [((128, WIDE), BF16), ((TOK, WIDTH), BF16), ((TOK, 128), F32)],
        near, recvs[4], spans[4], qt, cum, weight, gate_values, norm_gain[None, :], out_weight,
        flops=10**9, name="project",
    )
    (mine,) = call(own_rows_kernel, [((128, WIDE), BF16)], feat, square, out_weight, flops=10**9, name="own_rows")
    recv = lax.ppermute(theirs, "head", [(g, g ^ 1) for g in range(8)])
    own, *sends = call(
        pair_kernel,
        [((32, WIDE), F32)] + [((32, WIDE), BF16)] * 3,
        mine, recv, flops=10**6, name="pair",
    )
    got = [lax.ppermute(sends[k - 1], "head", [(g, g ^ (2 * k)) for g in range(8)]) for k in (3, 2, 1)]
    (out,) = call(final_kernel, [((32, DM), BF16)], own, *got, flops=10**6, name="final")
    return out


def solution(mesh):
    placed = (
        P("seq", "head"),
        P("seq", "head"),
        P("seq", None),
        P("seq", None),
        P("seq", "head"),
        P("seq", "head"),
        P("seq", "head", None),
        P("head"),
        P("head"),
        P("head", None),
    )
    return jax.shard_map(
        on_device, mesh=mesh, in_specs=placed, out_specs=P(("seq", "head"), None), check_vma=False
    )
```

```python
import jax
import jax.numpy as jnp
from jax import lax
from jax.experimental import pallas as pl
from jax.experimental.pallas import tpu as pltpu
from jax.sharding import PartitionSpec as P

H = 80
HEADS = 10
P_SIZE = 64
N = 128
TOK = 256
WIDTH = HEADS * P_SIZE
DM = 2560
WIDE = DM + 128
LOCAL_LEVELS = 9
PAY = WIDTH + 32

EPSILON = 1e-05

F32 = jnp.float32
BF16 = jnp.bfloat16


def dot(a, b):
    return jnp.dot(a, b, preferred_element_type=F32)


def split_two(value):
    high = value.astype(BF16)
    return high, (value - high.astype(F32)).astype(BF16)


def pad_heads(value):
    return jnp.concatenate([value, jnp.zeros((16 - HEADS, value.shape[1]), F32)], axis=0)


def fetch(sources, targets, sems):
    copies = [pltpu.make_async_copy(s, t, sems.at[i]) for i, (s, t) in enumerate(zip(sources, targets))]
    for copy in copies:
        copy.start()
    return copies


def put_totals(pay_ref, total):
    high, low = split_two(total)
    pay_ref[WIDTH : WIDTH + 16, :] = high
    pay_ref[WIDTH + 16 : WIDTH + 32, :] = low


def totals_of(recv_ref):
    return recv_ref[WIDTH : WIDTH + 16, :].astype(F32) + recv_ref[WIDTH + 16 : WIDTH + 32, :].astype(F32)


def state_kernel(
    x_in, k_in, step_in, decay_in, pay_ref, state_ref, xt_ref, cum_ref, tot_ref,
    x_ref, k_ref, step_ref, decay_ref, sems,
):
    copies = fetch((decay_in, step_in, k_in, x_in), (decay_ref, step_ref, k_ref, x_ref), sems)
    copies[0].wait()
    copies[1].wait()
    decay = pad_heads(decay_ref[...])
    step = pad_heads(step_ref[...])
    high = decay.astype(BF16)
    rest = decay - high.astype(F32)
    mid, low = split_two(rest)
    earlier = lax.broadcasted_iota(jnp.int32, (TOK, TOK), 0)
    later = lax.broadcasted_iota(jnp.int32, (TOK, TOK), 1)
    upto = jnp.where(earlier <= later, 1.0, 0.0).astype(BF16)
    parts = dot(jnp.concatenate([high, mid, low], axis=0), upto)
    cum = parts[0:16] + parts[16:32] + parts[32:48]
    total = jnp.broadcast_to(cum[:, TOK - 1 : TOK], (16, 128))
    cum_ref[...] = cum
    tot_ref[...] = total
    put_totals(pay_ref, total)
    coef = step * jnp.exp(cum[:, TOK - 1 : TOK] - cum)
    copies[2].wait()
    copies[3].wait()
    keys = k_ref[...]
    for j in range(WIDTH // 128):
        rows = slice(j * 128, (j + 1) * 128)
        xt = x_ref[:, rows].astype(F32).T
        xt_ref[rows, :] = xt.astype(BF16)
        scaled = jnp.concatenate(
            [xt[0:64] * coef[2 * j : 2 * j + 1], xt[64:128] * coef[2 * j + 1 : 2 * j + 2]], axis=0
        )
        state = dot(scaled.astype(BF16), keys)
        state_ref[rows, :] = state
        pay_ref[rows, :] = state.astype(BF16)


def local_kernel(
    xt_ref, cum_ref, skip_ref, k_in, q_in, step_in, w_in, out_ref, qt_ref,
    k_ref, q_ref, step_ref, w_ref, sems,
):
    copies = fetch((q_in, k_in, step_in, w_in), (q_ref, k_ref, step_ref, w_ref), sems)
    copies[0].wait()
    copies[1].wait()
    qt = q_ref[...].astype(F32).T.astype(BF16)
    qt_ref[...] = qt
    scores = dot(k_ref[...], qt)
    cum = cum_ref[...]
    cols = cum.T
    early = lax.broadcasted_iota(jnp.int32, (128, 128), 0)
    late = lax.broadcasted_iota(jnp.int32, (128, 128), 1)
    differ = jnp.bitwise_xor(early, late)
    level = jnp.zeros((128, 128), jnp.int32)
    for shift in range(7):
        level = level + (differ >= 1 << shift).astype(jnp.int32)
    level = jnp.where(early <= late, level, -1)
    copies[2].wait()
    copies[3].wait()
    for h in range(HEADS):
        weights = w_ref[h, 0:LOCAL_LEVELS, :].astype(F32)
        xt = xt_ref[h * 64 : (h + 1) * 64, :].astype(F32)
        inputs = (xt * step_ref[h : h + 1, :]).astype(BF16)

        def faded(i, j):
            s, t = slice(i * 128, (i + 1) * 128), slice(j * 128, (j + 1) * 128)
            gap = jnp.minimum(cum[h : h + 1, t] - cols[s, h : h + 1], 0.0)
            return jnp.exp(gap) * scores[s, t]

        def diagonal(i):
            t = slice(i * 128, (i + 1) * 128)
            picked = jnp.zeros((128, 128), F32)
            for l in range(LOCAL_LEVELS - 1):
                picked = jnp.where(level == l, weights[l : l + 1, t], picked)
            return (faded(i, i) * picked).astype(BF16)

        first = diagonal(0)
        second = jnp.concatenate(
            [(faded(0, 1) * weights[8:9, 128:256]).astype(BF16), diagonal(1)], axis=0
        )
        mixed = jnp.concatenate([dot(inputs[:, 0:128], first), dot(inputs, second)], axis=1)
        out_ref[h * 64 : (h + 1) * 64, :] = mixed + skip_ref[h] * xt


def combine_kernel(bit, state_ref, tot_ref, span_ref, recv_ref, pay_ref, new_ref, ntot_ref, nspan_ref):
    upper = ((lax.axis_index("seq") >> bit) & 1) > 0
    total = tot_ref[...]
    other = totals_of(recv_ref)
    new_total = total + other
    ntot_ref[...] = new_total
    nspan_ref[...] = span_ref[...] + jnp.where(upper, other, 0.0)
    put_totals(pay_ref, new_total)
    for_other = jnp.where(upper, jnp.exp(total), 1.0)
    for_mine = jnp.where(upper, 1.0, jnp.exp(other))
    for h in range(HEADS):
        rows = slice(h * 64, (h + 1) * 64)
        new = for_other[h : h + 1] * recv_ref[rows, :].astype(F32) + for_mine[h : h + 1] * state_ref[rows, :]
        new_ref[rows, :] = new
        pay_ref[rows, :] = new.astype(BF16)


def quad_kernel(_, r3, r2, r1, state_ref, tot_ref, pay_ref, near_ref, pair_ref, new_ref, ntot_ref, span1_ref, span2_ref):
    x = lax.axis_index("seq")
    odd, upper = (x & 1) > 0, (x & 2) > 0
    near_ref[...] = r1[0:WIDTH, :]
    t0 = tot_ref[...]
    t1, t2, t3 = totals_of(r1), totals_of(r2), totals_of(r3)
    total = t0 + t1 + t2 + t3
    ntot_ref[...] = total
    put_totals(pay_ref, total)
    span1 = jnp.where(odd, t1, 0.0)
    span1_ref[...] = span1
    span2_ref[...] = span1 + jnp.where(upper, t2 + t3, 0.0)
    mine_to = jnp.where(odd, 0.0, t1)
    next_to = jnp.where(odd, t0, 0.0)
    across_to = jnp.where(odd, 0.0, t3)
    far_to = jnp.where(odd, t2, 0.0)
    lower_pair = jnp.exp(jnp.where(upper, t0 + t1, 0.0))
    f2, f3 = jnp.exp(across_to), jnp.exp(far_to)
    other = jnp.where(upper, 0.0, t2 + t3)
    f0, f1 = jnp.exp(mine_to + other), jnp.exp(next_to + other)
    for h in range(HEADS):
        rows = slice(h * 64, (h + 1) * 64)
        row = slice(h, h + 1)
        pair = f2[row] * r2[rows, :].astype(F32) + f3[row] * r3[rows, :].astype(F32)
        pair_ref[rows, :] = pair.astype(BF16)
        new = f0[row] * state_ref[rows, :] + f1[row] * r1[rows, :].astype(F32) + lower_pair[row] * pair
        new_ref[rows, :] = new
        pay_ref[rows, :] = new.astype(BF16)


def last_combine_kernel(state_ref, tot_ref, span_ref, recv_ref, pay_ref, nspan_ref):
    upper = ((lax.axis_index("seq") >> 3) & 1) > 0
    total = tot_ref[...]
    other = totals_of(recv_ref)
    nspan_ref[...] = span_ref[...] + jnp.where(upper, other, 0.0)
    for_other = jnp.where(upper, jnp.exp(total), 1.0)
    for_mine = jnp.where(upper, 1.0, jnp.exp(other))
    for h in range(HEADS):
        rows = slice(h * 64, (h + 1) * 64)
        new = for_other[h : h + 1] * recv_ref[rows, :].astype(F32) + for_mine[h : h + 1] * state_ref[rows, :]
        pay_ref[rows, :] = new.astype(BF16)


def far_term(recv_ref, qt, h, coef):
    rows = slice(h * 64, (h + 1) * 64)
    return dot(recv_ref[rows, :], qt) * coef


def far_coef(bit, cum, span_ref, w_ref, h):
    upper = ((lax.axis_index("seq") >> bit) & 1) > 0
    lift = jnp.exp(cum[h : h + 1, :] + span_ref[h : h + 1, 0:1])
    weight = w_ref[h, LOCAL_LEVELS + bit : LOCAL_LEVELS + bit + 1, :].astype(F32)
    return jnp.where(upper, lift * weight, 0.0)


def near_kernel(local_ref, r0, r1, r2, r3, s0, s1, s2, s3, s4, qt_ref, cum_ref, w_ref, gate_ref, near_ref, lift_ref):
    qt = qt_ref[...]
    cum = cum_ref[...]
    for j in range(WIDTH // 128):
        cols = slice(j * 128, (j + 1) * 128)
        totals, lifts = [], []
        for h in (2 * j, 2 * j + 1):
            total = local_ref[h * 64 : (h + 1) * 64, :]
            for bit, (recv, span) in enumerate(((r0, s0), (r1, s1), (r2, s2), (r3, s3))):
                total = total + far_term(recv, qt, h, far_coef(bit, cum, span, w_ref, h))
            totals.append(total)
            lifts.append(jnp.broadcast_to(far_coef(4, cum, s4, w_ref, h), (64, TOK)))
        gate = gate_ref[:, cols].astype(F32)
        gate = gate / (1.0 + jnp.exp(-gate))
        near_ref[:, cols] = jnp.concatenate(totals, axis=0).T * gate
        lift_ref[:, cols] = jnp.concatenate(lifts, axis=0).T * gate


def feature_kernel(near_ref, lift_ref, recv_ref, q_ref, gain_ref, ow_ref, theirs_ref, feat_ref, square_ref):
    query = q_ref[...]
    squares = jnp.zeros((TOK, 1), F32)
    for j in range(WIDTH // 128):
        cols = slice(j * 128, (j + 1) * 128)
        far = lax.dot_general(query, recv_ref[cols, :], (((1,), (1,)), ((), ())), preferred_element_type=F32)
        gated = near_ref[:, cols] + lift_ref[:, cols] * far
        squares = squares + jnp.sum(gated * gated, axis=1, keepdims=True)
        feat_ref[:, cols] = (gated * gain_ref[:, cols]).astype(BF16)
    square_ref[...] = jnp.broadcast_to(squares, (TOK, 128))
    product_rows(feat_ref, square_ref, ow_ref, theirs_ref, 1 - (lax.axis_index("head") & 1))


def product_rows(feat_ref, square_ref, ow_ref, out_ref, side):
    lane = lax.broadcasted_iota(jnp.int32, (32, 128), 1)
    starts = [pl.multiple_of((2 * y + side) * 32, 32) for y in range(4)]
    rows = jnp.concatenate([feat_ref[pl.ds(s, 32), :] for s in starts], axis=0)
    out_ref[:, 0:DM] = dot(rows, ow_ref[...]).astype(BF16)
    for y, s in enumerate(starts):
        high, low = split_two(square_ref[pl.ds(s, 32), :])
        out_ref[y * 32 : (y + 1) * 32, DM:WIDE] = jnp.where(
            lane < 64, high.astype(F32), low.astype(F32)
        ).astype(BF16)


def own_rows_kernel(feat_ref, square_ref, ow_ref, mine_ref):
    product_rows(feat_ref, square_ref, ow_ref, mine_ref, lax.axis_index("head") & 1)


def squares_at(ref, rows, at):
    return ref[rows, at : at + 1].astype(F32) + ref[rows, at + 64 : at + 65].astype(F32)


def pair_kernel(mine_ref, recv_ref, own_ref, o1, o2, o3):
    y = lax.axis_index("head") >> 1
    lane = lax.broadcasted_iota(jnp.int32, (32, 128), 1)
    for k, out_ref in enumerate((own_ref, o1, o2, o3)):
        rows = pl.ds(pl.multiple_of(jnp.bitwise_xor(y, k) * 32, 32), 32)
        total = mine_ref[rows, 0:DM].astype(F32) + recv_ref[rows, 0:DM].astype(F32)
        out_ref[:, 0:DM] = total.astype(out_ref.dtype)
        square = jnp.broadcast_to(squares_at(mine_ref, rows, DM) + squares_at(recv_ref, rows, DM), (32, 128))
        high, low = split_two(square)
        out_ref[:, DM:WIDE] = jnp.where(lane < 64, high.astype(F32), low.astype(F32)).astype(out_ref.dtype)


def final_kernel(own_ref, r1, r2, r3, out_ref):
    every = slice(0, 32)
    square = sum(squares_at(ref, every, DM) for ref in (own_ref, r1, r2, r3))
    scale = lax.rsqrt(square * (1.0 / (H * P_SIZE)) + EPSILON)
    total = own_ref[:, 0:DM].astype(F32)
    for ref in (r1, r2, r3):
        total = total + ref[:, 0:DM].astype(F32)
    out_ref[...] = (total * scale).astype(BF16)


def call(kernel, outs, *args, scratch=(), flops=0, name=None, smem=(), hbm=(), free=()):
    def space(i):
        if i in smem:
            return pltpu.SMEM
        if i in hbm:
            return pltpu.HBM
        return pl.ANY if i in free else pltpu.VMEM

    specs = [pl.BlockSpec(memory_space=space(i)) for i in range(len(args))]
    args = [pltpu.with_memory_space_constraint(a, pltpu.HBM) if i in hbm else a for i, a in enumerate(args)]
    shapes = [jax.ShapeDtypeStruct(shape, dtype) for shape, dtype in outs]
    outputs = pl.pallas_call(
        kernel,
        out_shape=shapes,
        in_specs=specs,
        out_specs=[pl.BlockSpec(memory_space=pltpu.VMEM) for _ in outs],
        scratch_shapes=list(scratch),
        compiler_params=pltpu.CompilerParams(vmem_limit_bytes=48 << 20),
        cost_estimate=pl.CostEstimate(flops=flops, transcendentals=0, bytes_accessed=flops // 100),
        name=name,
    )(*args)
    return outputs


def on_device(token_values, gate_values, state_in, state_out, step_size, log_decay, level_weight, skip_weight, norm_gain, out_weight):
    step = jnp.transpose(step_size)
    decay = jnp.transpose(log_decay)
    weight = jnp.transpose(level_weight, (1, 2, 0))
    pay, state, xt, cum, total = call(
        state_kernel,
        [((PAY, N), BF16), ((WIDTH, N), F32), ((WIDTH, TOK), BF16), ((16, TOK), F32), ((16, 128), F32)],
        token_values, state_in, step, decay, flops=10**8, name="state", hbm=(0, 1, 2, 3),
        scratch=[
            pltpu.VMEM((TOK, WIDTH), BF16), pltpu.VMEM((TOK, N), BF16), pltpu.VMEM((HEADS, TOK), F32),
            pltpu.VMEM((HEADS, TOK), F32), pltpu.SemaphoreType.DMA((4,)),
        ],
    )
    local, qt = call(
        local_kernel,
        [((WIDTH, TOK), F32), ((N, TOK), BF16)],
        xt, cum, skip_weight, state_in, state_out, step, weight,
        flops=5 * 10**9, name="local", smem=(2,), hbm=(3, 4, 5, 6),
        scratch=[
            pltpu.VMEM((TOK, N), BF16), pltpu.VMEM((TOK, N), BF16), pltpu.VMEM((HEADS, TOK), F32),
            pltpu.VMEM((HEADS, 14, TOK), BF16), pltpu.SemaphoreType.DMA((4,)),
        ],
    )
    r3, r2, r1 = [lax.ppermute(pay, "seq", [(d, d ^ k) for d in range(32)]) for k in (3, 2, 1)]
    pay, next_state, pair, state, total, span1, span2 = call(
        quad_kernel,
        [((PAY, N), BF16), ((WIDTH, N), BF16), ((WIDTH, N), BF16), ((WIDTH, N), F32)] + [((16, 128), F32)] * 3,
        local, r3, r2, r1, state, total, flops=10**6, name="quad", free=(0,),
    )
    recvs, spans = [next_state, pair], [jnp.zeros((16, 128), F32), span1, span2]
    recvs.append(lax.ppermute(pay, "seq", [(d, d ^ 4) for d in range(32)]))
    pay, state, total, span = call(
        lambda *refs: combine_kernel(2, *refs),
        [((PAY, N), BF16), ((WIDTH, N), F32), ((16, 128), F32), ((16, 128), F32)],
        state, total, span2, recvs[2], flops=10**6, name="combine",
    )
    spans.append(span)
    recvs.append(lax.ppermute(pay, "seq", [(d, d ^ 12) for d in range(32)]))
    pay, span = call(
        last_combine_kernel, [((WIDTH, N), BF16), ((16, 128), F32)],
        state, total, span, recvs[3], flops=10**6, name="combine",
    )
    spans.append(span)
    recvs.append(lax.ppermute(pay, "seq", [(d, d ^ 28) for d in range(32)]))
    near, lift = call(
        near_kernel, [((TOK, WIDTH), F32)] * 2,
        local, *recvs[:4], *spans, qt, cum, weight, gate_values,
        flops=2 * 10**9, name="near",
    )
    theirs, feat, square = call(
        feature_kernel,
        [((128, WIDE), BF16), ((TOK, WIDTH), BF16), ((TOK, 128), F32)],
        near, lift, recvs[4], state_out, norm_gain[None, :], out_weight,
        flops=10**9, name="feature",
    )
    (mine,) = call(own_rows_kernel, [((128, WIDE), BF16)], feat, square, out_weight, flops=10**9, name="own_rows")
    recv = lax.ppermute(theirs, "head", [(g, g ^ 1) for g in range(8)])
    own, *sends = call(
        pair_kernel,
        [((32, WIDE), F32)] + [((32, WIDE), BF16)] * 3,
        mine, recv, flops=10**6, name="pair",
    )
    got = [lax.ppermute(sends[k - 1], "head", [(g, g ^ (2 * k)) for g in range(8)]) for k in (3, 2, 1)]
    (out,) = call(final_kernel, [((32, DM), BF16)], own, *got, flops=10**6, name="final")
    return out


def solution(mesh):
    placed = (
        P("seq", "head"),
        P("seq", "head"),
        P("seq", None),
        P("seq", None),
        P("seq", "head"),
        P("seq", "head"),
        P("seq", "head", None),
        P("head"),
        P("head"),
        P("head", None),
    )
    return jax.shard_map(
        on_device, mesh=mesh, in_specs=placed, out_specs=P(("seq", "head"), None), check_vma=False
    )
```

```python
import jax
import jax.numpy as jnp
from jax import lax
from jax.experimental import pallas as pl
from jax.experimental.pallas import tpu as pltpu
from jax.sharding import PartitionSpec as P

H = 80
HEADS = 10
P_SIZE = 64
N = 128
TOK = 256
WIDTH = HEADS * P_SIZE
DM = 2560
WIDE = DM + 128
LOCAL_LEVELS = 9
PAY = WIDTH + 32

EPSILON = 1e-05

F32 = jnp.float32
BF16 = jnp.bfloat16


def dot(a, b):
    return jnp.dot(a, b, preferred_element_type=F32)


def split_two(value):
    high = value.astype(BF16)
    return high, (value - high.astype(F32)).astype(BF16)


def pad_heads(value):
    return jnp.concatenate([value, jnp.zeros((16 - HEADS, value.shape[1]), F32)], axis=0)


def fetch(sources, targets, sems):
    copies = [pltpu.make_async_copy(s, t, sems.at[i]) for i, (s, t) in enumerate(zip(sources, targets))]
    for copy in copies:
        copy.start()
    return copies


def put_totals(pay_ref, total):
    high, low = split_two(total)
    pay_ref[WIDTH : WIDTH + 16, :] = high
    pay_ref[WIDTH + 16 : WIDTH + 32, :] = low


def totals_of(recv_ref):
    return recv_ref[WIDTH : WIDTH + 16, :].astype(F32) + recv_ref[WIDTH + 16 : WIDTH + 32, :].astype(F32)


def state_kernel(
    x_in, k_in, step_in, decay_in, pay_ref, state_ref, xt_ref, cum_ref, tot_ref,
    x_ref, k_ref, step_ref, decay_ref, sems,
):
    copies = fetch((decay_in, step_in, k_in, x_in), (decay_ref, step_ref, k_ref, x_ref), sems)
    copies[0].wait()
    copies[1].wait()
    decay = pad_heads(decay_ref[...])
    step = pad_heads(step_ref[...])
    high = decay.astype(BF16)
    rest = decay - high.astype(F32)
    mid, low = split_two(rest)
    earlier = lax.broadcasted_iota(jnp.int32, (TOK, TOK), 0)
    later = lax.broadcasted_iota(jnp.int32, (TOK, TOK), 1)
    upto = jnp.where(earlier <= later, 1.0, 0.0).astype(BF16)
    parts = dot(jnp.concatenate([high, mid, low], axis=0), upto)
    cum = parts[0:16] + parts[16:32] + parts[32:48]
    total = jnp.broadcast_to(cum[:, TOK - 1 : TOK], (16, 128))
    cum_ref[...] = cum
    tot_ref[...] = total
    put_totals(pay_ref, total)
    coef = step * jnp.exp(cum[:, TOK - 1 : TOK] - cum)
    copies[2].wait()
    copies[3].wait()
    keys = k_ref[...]
    for j in range(WIDTH // 128):
        rows = slice(j * 128, (j + 1) * 128)
        xt = x_ref[:, rows].astype(F32).T
        xt_ref[rows, :] = xt.astype(BF16)
        scaled = jnp.concatenate(
            [xt[0:64] * coef[2 * j : 2 * j + 1], xt[64:128] * coef[2 * j + 1 : 2 * j + 2]], axis=0
        )
        state = dot(scaled.astype(BF16), keys)
        state_ref[rows, :] = state
        pay_ref[rows, :] = state.astype(BF16)


def local_kernel(
    xt_ref, cum_ref, skip_ref, k_in, q_in, step_in, w_in, out_ref, qt_ref,
    k_ref, q_ref, step_ref, w_ref, sems,
):
    copies = fetch((q_in, k_in, step_in, w_in), (q_ref, k_ref, step_ref, w_ref), sems)
    copies[0].wait()
    copies[1].wait()
    qt = q_ref[...].astype(F32).T.astype(BF16)
    qt_ref[...] = qt
    scores = dot(k_ref[...], qt)
    cum = cum_ref[...]
    cols = cum.T
    early = lax.broadcasted_iota(jnp.int32, (128, 128), 0)
    late = lax.broadcasted_iota(jnp.int32, (128, 128), 1)
    differ = jnp.bitwise_xor(early, late)
    level = jnp.zeros((128, 128), jnp.int32)
    for shift in range(7):
        level = level + (differ >= 1 << shift).astype(jnp.int32)
    level = jnp.where(early <= late, level, -1)
    copies[2].wait()
    copies[3].wait()
    for h in range(HEADS):
        weights = w_ref[h, 0:LOCAL_LEVELS, :].astype(F32)
        xt = xt_ref[h * 64 : (h + 1) * 64, :].astype(F32)
        inputs = (xt * step_ref[h : h + 1, :]).astype(BF16)

        def faded(i, j):
            s, t = slice(i * 128, (i + 1) * 128), slice(j * 128, (j + 1) * 128)
            gap = jnp.minimum(cum[h : h + 1, t] - cols[s, h : h + 1], 0.0)
            return jnp.exp(gap) * scores[s, t]

        def diagonal(i):
            t = slice(i * 128, (i + 1) * 128)
            picked = jnp.zeros((128, 128), F32)
            for l in range(LOCAL_LEVELS - 1):
                picked = jnp.where(level == l, weights[l : l + 1, t], picked)
            return (faded(i, i) * picked).astype(BF16)

        first = diagonal(0)
        second = jnp.concatenate(
            [(faded(0, 1) * weights[8:9, 128:256]).astype(BF16), diagonal(1)], axis=0
        )
        mixed = jnp.concatenate([dot(inputs[:, 0:128], first), dot(inputs, second)], axis=1)
        out_ref[h * 64 : (h + 1) * 64, :] = mixed + skip_ref[h] * xt


def combine_kernel(bit, state_ref, tot_ref, span_ref, recv_ref, pay_ref, new_ref, ntot_ref, nspan_ref):
    upper = ((lax.axis_index("seq") >> bit) & 1) > 0
    total = tot_ref[...]
    other = totals_of(recv_ref)
    new_total = total + other
    ntot_ref[...] = new_total
    nspan_ref[...] = span_ref[...] + jnp.where(upper, other, 0.0)
    put_totals(pay_ref, new_total)
    for_other = jnp.where(upper, jnp.exp(total), 1.0)
    for_mine = jnp.where(upper, 1.0, jnp.exp(other))
    for h in range(HEADS):
        rows = slice(h * 64, (h + 1) * 64)
        new = for_other[h : h + 1] * recv_ref[rows, :].astype(F32) + for_mine[h : h + 1] * state_ref[rows, :]
        new_ref[rows, :] = new
        pay_ref[rows, :] = new.astype(BF16)


def quad_kernel(_, r3, r2, r1, state_ref, tot_ref, pay_ref, near_ref, pair_ref, new_ref, ntot_ref, span1_ref, span2_ref):
    x = lax.axis_index("seq")
    odd, upper = (x & 1) > 0, (x & 2) > 0
    near_ref[...] = r1[0:WIDTH, :]
    t0 = tot_ref[...]
    t1, t2, t3 = totals_of(r1), totals_of(r2), totals_of(r3)
    total = t0 + t1 + t2 + t3
    ntot_ref[...] = total
    put_totals(pay_ref, total)
    span1 = jnp.where(odd, t1, 0.0)
    span1_ref[...] = span1
    span2_ref[...] = span1 + jnp.where(upper, t2 + t3, 0.0)
    mine_to = jnp.where(odd, 0.0, t1)
    next_to = jnp.where(odd, t0, 0.0)
    across_to = jnp.where(odd, 0.0, t3)
    far_to = jnp.where(odd, t2, 0.0)
    lower_pair = jnp.exp(jnp.where(upper, t0 + t1, 0.0))
    f2, f3 = jnp.exp(across_to), jnp.exp(far_to)
    other = jnp.where(upper, 0.0, t2 + t3)
    f0, f1 = jnp.exp(mine_to + other), jnp.exp(next_to + other)
    for h in range(HEADS):
        rows = slice(h * 64, (h + 1) * 64)
        row = slice(h, h + 1)
        pair = f2[row] * r2[rows, :].astype(F32) + f3[row] * r3[rows, :].astype(F32)
        pair_ref[rows, :] = pair.astype(BF16)
        new = f0[row] * state_ref[rows, :] + f1[row] * r1[rows, :].astype(F32) + lower_pair[row] * pair
        new_ref[rows, :] = new
        pay_ref[rows, :] = new.astype(BF16)


def last_combine_kernel(state_ref, tot_ref, span_ref, recv_ref, pay_ref, nspan_ref):
    upper = ((lax.axis_index("seq") >> 3) & 1) > 0
    total = tot_ref[...]
    other = totals_of(recv_ref)
    nspan_ref[...] = span_ref[...] + jnp.where(upper, other, 0.0)
    for_other = jnp.where(upper, jnp.exp(total), 1.0)
    for_mine = jnp.where(upper, 1.0, jnp.exp(other))
    for h in range(HEADS):
        rows = slice(h * 64, (h + 1) * 64)
        new = for_other[h : h + 1] * recv_ref[rows, :].astype(F32) + for_mine[h : h + 1] * state_ref[rows, :]
        pay_ref[rows, :] = new.astype(BF16)


def far_term(recv_ref, qt, h, coef):
    rows = slice(h * 64, (h + 1) * 64)
    return dot(recv_ref[rows, :], qt) * coef


def far_coef(bit, cum, span_ref, w_ref, h):
    upper = ((lax.axis_index("seq") >> bit) & 1) > 0
    lift = jnp.exp(cum[h : h + 1, :] + span_ref[h : h + 1, 0:1])
    weight = w_ref[h, LOCAL_LEVELS + bit : LOCAL_LEVELS + bit + 1, :].astype(F32)
    return jnp.where(upper, lift * weight, 0.0)


def near_kernel(local_ref, r0, r1, r2, r3, s0, s1, s2, s3, s4, qt_ref, cum_ref, w_ref, gate_ref, near_ref, lift_ref):
    qt = qt_ref[...]
    cum = cum_ref[...]
    for j in range(WIDTH // 128):
        cols = slice(j * 128, (j + 1) * 128)
        totals, lifts = [], []
        for h in (2 * j, 2 * j + 1):
            total = local_ref[h * 64 : (h + 1) * 64, :]
            for bit, (recv, span) in enumerate(((r0, s0), (r1, s1), (r2, s2), (r3, s3))):
                total = total + far_term(recv, qt, h, far_coef(bit, cum, span, w_ref, h))
            totals.append(total)
            lifts.append(jnp.broadcast_to(far_coef(4, cum, s4, w_ref, h), (64, TOK)))
        gate = gate_ref[:, cols].astype(F32)
        gate = gate / (1.0 + jnp.exp(-gate))
        near_ref[:, cols] = jnp.concatenate(totals, axis=0).T * gate
        lift_ref[:, cols] = jnp.concatenate(lifts, axis=0).T * gate


def feature_kernel(near_ref, lift_ref, recv_ref, q_ref, gain_ref, ow_ref, first_ref, second_ref, feat_ref, square_ref):
    query = q_ref[...]
    squares = jnp.zeros((TOK, 1), F32)
    for j in range(WIDTH // 128):
        cols = slice(j * 128, (j + 1) * 128)
        far = lax.dot_general(query, recv_ref[cols, :], (((1,), (1,)), ((), ())), preferred_element_type=F32)
        gated = near_ref[:, cols] + lift_ref[:, cols] * far
        squares = squares + jnp.sum(gated * gated, axis=1, keepdims=True)
        feat_ref[:, cols] = (gated * gain_ref[:, cols]).astype(BF16)
    square_ref[...] = jnp.broadcast_to(squares, (TOK, 128))
    product_rows(feat_ref, square_ref, ow_ref, first_ref, second_ref, 1 - (lax.axis_index("head") & 1))


def product_rows(feat_ref, square_ref, ow_ref, first_ref, second_ref, side):
    y = lax.axis_index("head") >> 1
    lane = lax.broadcasted_iota(jnp.int32, (32, 128), 1)
    starts = [pl.multiple_of((2 * jnp.bitwise_xor(y, k) + side) * 32, 32) for k in (3, 2, 1, 0)]
    rows = jnp.concatenate([feat_ref[pl.ds(s, 32), :] for s in starts], axis=0)
    product = dot(rows, ow_ref[...]).astype(BF16)
    first_ref[:, 0:DM] = product[0:64]
    second_ref[:, 0:DM] = product[64:128]
    for i, s in enumerate(starts):
        high, low = split_two(square_ref[pl.ds(s, 32), :])
        out_ref = first_ref if i < 2 else second_ref
        out_ref[(i % 2) * 32 : (i % 2 + 1) * 32, DM:WIDE] = jnp.where(
            lane < 64, high.astype(F32), low.astype(F32)
        ).astype(BF16)


def own_rows_kernel(feat_ref, square_ref, ow_ref, first_ref, second_ref):
    product_rows(feat_ref, square_ref, ow_ref, first_ref, second_ref, lax.axis_index("head") & 1)


def squares_at(ref, rows, at):
    return ref[rows, at : at + 1].astype(F32) + ref[rows, at + 64 : at + 65].astype(F32)


def pair_kernel(mine_ref, recv_ref, *out_refs):
    lane = lax.broadcasted_iota(jnp.int32, (32, 128), 1)
    for i, out_ref in enumerate(out_refs):
        rows = slice(i * 32, (i + 1) * 32)
        total = mine_ref[rows, 0:DM].astype(F32) + recv_ref[rows, 0:DM].astype(F32)
        out_ref[:, 0:DM] = total.astype(out_ref.dtype)
        square = jnp.broadcast_to(squares_at(mine_ref, rows, DM) + squares_at(recv_ref, rows, DM), (32, 128))
        high, low = split_two(square)
        out_ref[:, DM:WIDE] = jnp.where(lane < 64, high.astype(F32), low.astype(F32)).astype(out_ref.dtype)


def final_kernel(own_ref, r1, r2, r3, out_ref):
    every = slice(0, 32)
    square = sum(squares_at(ref, every, DM) for ref in (own_ref, r1, r2, r3))
    scale = lax.rsqrt(square * (1.0 / (H * P_SIZE)) + EPSILON)
    total = own_ref[:, 0:DM].astype(F32)
    for ref in (r1, r2, r3):
        total = total + ref[:, 0:DM].astype(F32)
    out_ref[...] = (total * scale).astype(BF16)


def call(kernel, outs, *args, scratch=(), flops=0, name=None, smem=(), hbm=(), free=()):
    def space(i):
        if i in smem:
            return pltpu.SMEM
        if i in hbm:
            return pltpu.HBM
        return pl.ANY if i in free else pltpu.VMEM

    specs = [pl.BlockSpec(memory_space=space(i)) for i in range(len(args))]
    args = [pltpu.with_memory_space_constraint(a, pltpu.HBM) if i in hbm else a for i, a in enumerate(args)]
    shapes = [jax.ShapeDtypeStruct(shape, dtype) for shape, dtype in outs]
    outputs = pl.pallas_call(
        kernel,
        out_shape=shapes,
        in_specs=specs,
        out_specs=[pl.BlockSpec(memory_space=pltpu.VMEM) for _ in outs],
        scratch_shapes=list(scratch),
        compiler_params=pltpu.CompilerParams(vmem_limit_bytes=48 << 20),
        cost_estimate=pl.CostEstimate(flops=flops, transcendentals=0, bytes_accessed=flops // 100),
        name=name,
    )(*args)
    return outputs


def on_device(token_values, gate_values, state_in, state_out, step_size, log_decay, level_weight, skip_weight, norm_gain, out_weight):
    step = jnp.transpose(step_size)
    decay = jnp.transpose(log_decay)
    weight = jnp.transpose(level_weight, (1, 2, 0))
    pay, state, xt, cum, total = call(
        state_kernel,
        [((PAY, N), BF16), ((WIDTH, N), F32), ((WIDTH, TOK), BF16), ((16, TOK), F32), ((16, 128), F32)],
        token_values, state_in, step, decay, flops=10**8, name="state", hbm=(0, 1, 2, 3),
        scratch=[
            pltpu.VMEM((TOK, WIDTH), BF16), pltpu.VMEM((TOK, N), BF16), pltpu.VMEM((HEADS, TOK), F32),
            pltpu.VMEM((HEADS, TOK), F32), pltpu.SemaphoreType.DMA((4,)),
        ],
    )
    local, qt = call(
        local_kernel,
        [((WIDTH, TOK), F32), ((N, TOK), BF16)],
        xt, cum, skip_weight, state_in, state_out, step, weight,
        flops=5 * 10**9, name="local", smem=(2,), hbm=(3, 4, 5, 6),
        scratch=[
            pltpu.VMEM((TOK, N), BF16), pltpu.VMEM((TOK, N), BF16), pltpu.VMEM((HEADS, TOK), F32),
            pltpu.VMEM((HEADS, 14, TOK), BF16), pltpu.SemaphoreType.DMA((4,)),
        ],
    )
    r3, r2, r1 = [lax.ppermute(pay, "seq", [(d, d ^ k) for d in range(32)]) for k in (3, 2, 1)]
    pay, next_state, pair, state, total, span1, span2 = call(
        quad_kernel,
        [((PAY, N), BF16), ((WIDTH, N), BF16), ((WIDTH, N), BF16), ((WIDTH, N), F32)] + [((16, 128), F32)] * 3,
        local, r3, r2, r1, state, total, flops=10**6, name="quad", free=(0,),
    )
    recvs, spans = [next_state, pair], [jnp.zeros((16, 128), F32), span1, span2]
    recvs.append(lax.ppermute(pay, "seq", [(d, d ^ 4) for d in range(32)]))
    pay, state, total, span = call(
        lambda *refs: combine_kernel(2, *refs),
        [((PAY, N), BF16), ((WIDTH, N), F32), ((16, 128), F32), ((16, 128), F32)],
        state, total, span2, recvs[2], flops=10**6, name="combine",
    )
    spans.append(span)
    recvs.append(lax.ppermute(pay, "seq", [(d, d ^ 12) for d in range(32)]))
    pay, span = call(
        last_combine_kernel, [((WIDTH, N), BF16), ((16, 128), F32)],
        state, total, span, recvs[3], flops=10**6, name="combine",
    )
    spans.append(span)
    recvs.append(lax.ppermute(pay, "seq", [(d, d ^ 28) for d in range(32)]))
    near, lift = call(
        near_kernel, [((TOK, WIDTH), F32)] * 2,
        local, *recvs[:4], *spans, qt, cum, weight, gate_values,
        flops=2 * 10**9, name="near",
    )
    half = ((64, WIDE), BF16)
    *theirs, feat, square = call(
        feature_kernel,
        [half, half, ((TOK, WIDTH), BF16), ((TOK, 128), F32)],
        near, lift, recvs[4], state_out, norm_gain[None, :], out_weight,
        flops=10**9, name="feature",
    )
    mine = call(own_rows_kernel, [half, half], feat, square, out_weight, flops=10**9, name="own_rows")
    swap = [(g, g ^ 1) for g in range(8)]
    recv = [lax.ppermute(part, "head", swap) for part in theirs]
    one = ((32, WIDE), BF16)
    send3, send2 = call(pair_kernel, [one, one], mine[0], recv[0], flops=10**6, name="pair")
    send1, own = call(pair_kernel, [one, ((32, WIDE), F32)], mine[1], recv[1], flops=10**6, name="pair")
    got = [
        lax.ppermute(send, "head", [(g, g ^ (2 * k)) for g in range(8)])
        for k, send in ((3, send3), (2, send2), (1, send1))
    ]
    (out,) = call(final_kernel, [((32, DM), BF16)], own, *got, flops=10**6, name="final")
    return out


def solution(mesh):
    placed = (
        P("seq", "head"),
        P("seq", "head"),
        P("seq", None),
        P("seq", None),
        P("seq", "head"),
        P("seq", "head"),
        P("seq", "head", None),
        P("head"),
        P("head"),
        P("head", None),
    )
    return jax.shard_map(
        on_device, mesh=mesh, in_specs=placed, out_specs=P(("seq", "head"), None), check_vma=False
    )
```

```python
import jax
import jax.numpy as jnp
from jax import lax
from jax.experimental import pallas as pl
from jax.experimental.pallas import tpu as pltpu
from jax.sharding import PartitionSpec as P

H = 80
HEADS = 10
P_SIZE = 64
N = 128
TOK = 256
WIDTH = HEADS * P_SIZE
DM = 2560
WIDE = DM + 128
LOCAL_LEVELS = 9
PAY = WIDTH + 32

EPSILON = 1e-05

F32 = jnp.float32
BF16 = jnp.bfloat16


def dot(a, b):
    return jnp.dot(a, b, preferred_element_type=F32)


def split_two(value):
    high = value.astype(BF16)
    return high, (value - high.astype(F32)).astype(BF16)


def pad_heads(value):
    return jnp.concatenate([value, jnp.zeros((16 - HEADS, value.shape[1]), F32)], axis=0)


def fetch(sources, targets, sems):
    copies = [pltpu.make_async_copy(s, t, sems.at[i]) for i, (s, t) in enumerate(zip(sources, targets))]
    for copy in copies:
        copy.start()
    return copies


def put_totals(pay_ref, total):
    high, low = split_two(total)
    pay_ref[WIDTH : WIDTH + 16, :] = high
    pay_ref[WIDTH + 16 : WIDTH + 32, :] = low


def totals_of(recv_ref):
    return recv_ref[WIDTH : WIDTH + 16, :].astype(F32) + recv_ref[WIDTH + 16 : WIDTH + 32, :].astype(F32)


def state_kernel(
    x_in, k_in, step_in, decay_in, pay_ref, state_ref, xt_ref, cum_ref, tot_ref,
    x_ref, k_ref, step_ref, decay_ref, sems,
):
    copies = fetch((decay_in, step_in, k_in, x_in), (decay_ref, step_ref, k_ref, x_ref), sems)
    copies[0].wait()
    copies[1].wait()
    decay = pad_heads(decay_ref[...])
    step = pad_heads(step_ref[...])
    high = decay.astype(BF16)
    rest = decay - high.astype(F32)
    mid, low = split_two(rest)
    earlier = lax.broadcasted_iota(jnp.int32, (TOK, TOK), 0)
    later = lax.broadcasted_iota(jnp.int32, (TOK, TOK), 1)
    upto = jnp.where(earlier <= later, 1.0, 0.0).astype(BF16)
    parts = dot(jnp.concatenate([high, mid, low], axis=0), upto)
    cum = parts[0:16] + parts[16:32] + parts[32:48]
    total = jnp.broadcast_to(cum[:, TOK - 1 : TOK], (16, 128))
    cum_ref[...] = cum
    tot_ref[...] = total
    put_totals(pay_ref, total)
    coef = step * jnp.exp(cum[:, TOK - 1 : TOK] - cum)
    copies[2].wait()
    copies[3].wait()
    keys = k_ref[...]
    for j in range(WIDTH // 128):
        rows = slice(j * 128, (j + 1) * 128)
        xt = x_ref[:, rows].astype(F32).T
        xt_ref[rows, :] = xt.astype(BF16)
        scaled = jnp.concatenate(
            [xt[0:64] * coef[2 * j : 2 * j + 1], xt[64:128] * coef[2 * j + 1 : 2 * j + 2]], axis=0
        )
        state = dot(scaled.astype(BF16), keys)
        state_ref[rows, :] = state
        pay_ref[rows, :] = state.astype(BF16)


def local_kernel(
    xt_ref, cum_ref, skip_ref, k_in, q_in, step_in, w_in, out_ref, qt_ref,
    k_ref, q_ref, step_ref, w_ref, sems,
):
    copies = fetch((q_in, k_in, step_in, w_in), (q_ref, k_ref, step_ref, w_ref), sems)
    copies[0].wait()
    copies[1].wait()
    qt = q_ref[...].astype(F32).T.astype(BF16)
    qt_ref[...] = qt
    scores = dot(k_ref[...], qt)
    cum = cum_ref[...]
    cols = cum.T
    early = lax.broadcasted_iota(jnp.int32, (128, 128), 0)
    late = lax.broadcasted_iota(jnp.int32, (128, 128), 1)
    differ = jnp.bitwise_xor(early, late)
    level = jnp.zeros((128, 128), jnp.int32)
    for shift in range(7):
        level = level + (differ >= 1 << shift).astype(jnp.int32)
    level = jnp.where(early <= late, level, -1)
    copies[2].wait()
    copies[3].wait()
    for h in range(HEADS):
        weights = w_ref[h, 0:LOCAL_LEVELS, :].astype(F32)
        xt = xt_ref[h * 64 : (h + 1) * 64, :].astype(F32)
        inputs = (xt * step_ref[h : h + 1, :]).astype(BF16)

        def faded(i, j):
            s, t = slice(i * 128, (i + 1) * 128), slice(j * 128, (j + 1) * 128)
            gap = jnp.minimum(cum[h : h + 1, t] - cols[s, h : h + 1], 0.0)
            return jnp.exp(gap) * scores[s, t]

        def diagonal(i):
            t = slice(i * 128, (i + 1) * 128)
            picked = jnp.zeros((128, 128), F32)
            for l in range(LOCAL_LEVELS - 1):
                picked = jnp.where(level == l, weights[l : l + 1, t], picked)
            return (faded(i, i) * picked).astype(BF16)

        first = diagonal(0)
        second = jnp.concatenate(
            [(faded(0, 1) * weights[8:9, 128:256]).astype(BF16), diagonal(1)], axis=0
        )
        mixed = jnp.concatenate([dot(inputs[:, 0:128], first), dot(inputs, second)], axis=1)
        out_ref[h * 64 : (h + 1) * 64, :] = mixed + skip_ref[h] * xt


def combine_kernel(bit, state_ref, tot_ref, span_ref, recv_ref, pay_ref, new_ref, ntot_ref, nspan_ref):
    upper = ((lax.axis_index("seq") >> bit) & 1) > 0
    total = tot_ref[...]
    other = totals_of(recv_ref)
    new_total = total + other
    ntot_ref[...] = new_total
    nspan_ref[...] = span_ref[...] + jnp.where(upper, other, 0.0)
    put_totals(pay_ref, new_total)
    for_other = jnp.where(upper, jnp.exp(total), 1.0)
    for_mine = jnp.where(upper, 1.0, jnp.exp(other))
    for h in range(HEADS):
        rows = slice(h * 64, (h + 1) * 64)
        new = for_other[h : h + 1] * recv_ref[rows, :].astype(F32) + for_mine[h : h + 1] * state_ref[rows, :]
        new_ref[rows, :] = new
        pay_ref[rows, :] = new.astype(BF16)


def quad_kernel(_, r3, r2, r1, state_ref, tot_ref, pay_ref, near_ref, pair_ref, new_ref, ntot_ref, span1_ref, span2_ref):
    x = lax.axis_index("seq")
    odd, upper = (x & 1) > 0, (x & 2) > 0
    near_ref[...] = r1[0:WIDTH, :]
    t0 = tot_ref[...]
    t1, t2, t3 = totals_of(r1), totals_of(r2), totals_of(r3)
    total = t0 + t1 + t2 + t3
    ntot_ref[...] = total
    put_totals(pay_ref, total)
    span1 = jnp.where(odd, t1, 0.0)
    span1_ref[...] = span1
    span2_ref[...] = span1 + jnp.where(upper, t2 + t3, 0.0)
    mine_to = jnp.where(odd, 0.0, t1)
    next_to = jnp.where(odd, t0, 0.0)
    across_to = jnp.where(odd, 0.0, t3)
    far_to = jnp.where(odd, t2, 0.0)
    lower_pair = jnp.exp(jnp.where(upper, t0 + t1, 0.0))
    f2, f3 = jnp.exp(across_to), jnp.exp(far_to)
    other = jnp.where(upper, 0.0, t2 + t3)
    f0, f1 = jnp.exp(mine_to + other), jnp.exp(next_to + other)
    for h in range(HEADS):
        rows = slice(h * 64, (h + 1) * 64)
        row = slice(h, h + 1)
        pair = f2[row] * r2[rows, :].astype(F32) + f3[row] * r3[rows, :].astype(F32)
        pair_ref[rows, :] = pair.astype(BF16)
        new = f0[row] * state_ref[rows, :] + f1[row] * r1[rows, :].astype(F32) + lower_pair[row] * pair
        new_ref[rows, :] = new
        pay_ref[rows, :] = new.astype(BF16)


def last_combine_kernel(state_ref, tot_ref, span_ref, recv_ref, pay_ref, nspan_ref):
    upper = ((lax.axis_index("seq") >> 3) & 1) > 0
    total = tot_ref[...]
    other = totals_of(recv_ref)
    nspan_ref[...] = span_ref[...] + jnp.where(upper, other, 0.0)
    for_other = jnp.where(upper, jnp.exp(total), 1.0)
    for_mine = jnp.where(upper, 1.0, jnp.exp(other))
    for h in range(HEADS):
        rows = slice(h * 64, (h + 1) * 64)
        new = for_other[h : h + 1] * recv_ref[rows, :].astype(F32) + for_mine[h : h + 1] * state_ref[rows, :]
        pay_ref[rows, :] = new.astype(BF16)


def far_term(recv_ref, qt, h, coef):
    rows = slice(h * 64, (h + 1) * 64)
    return dot(recv_ref[rows, :], qt) * coef


def far_coef(bit, cum, span_ref, w_ref, h):
    upper = ((lax.axis_index("seq") >> bit) & 1) > 0
    lift = jnp.exp(cum[h : h + 1, :] + span_ref[h : h + 1, 0:1])
    weight = w_ref[h, LOCAL_LEVELS + bit : LOCAL_LEVELS + bit + 1, :].astype(F32)
    return jnp.where(upper, lift * weight, 0.0)


def near_kernel(local_ref, r0, r1, r2, r3, s0, s1, s2, s3, s4, qt_ref, cum_ref, w_ref, gate_ref, near_ref, lift_ref):
    qt = qt_ref[...]
    cum = cum_ref[...]
    for j in range(WIDTH // 128):
        cols = slice(j * 128, (j + 1) * 128)
        totals, lifts = [], []
        for h in (2 * j, 2 * j + 1):
            total = local_ref[h * 64 : (h + 1) * 64, :]
            for bit, (recv, span) in enumerate(((r0, s0), (r1, s1), (r2, s2), (r3, s3))):
                total = total + far_term(recv, qt, h, far_coef(bit, cum, span, w_ref, h))
            totals.append(total)
            lifts.append(jnp.broadcast_to(far_coef(4, cum, s4, w_ref, h), (64, TOK)))
        gate = gate_ref[:, cols].astype(F32)
        gate = gate / (1.0 + jnp.exp(-gate))
        near_ref[:, cols] = jnp.concatenate(totals, axis=0).T * gate
        lift_ref[:, cols] = jnp.concatenate(lifts, axis=0).T * gate


def feature_kernel(near_ref, lift_ref, recv_ref, q_ref, gain_ref, ow_ref, first_ref, second_ref, feat_ref, square_ref):
    query = q_ref[...]
    squares = jnp.zeros((TOK, 1), F32)
    for j in range(WIDTH // 128):
        cols = slice(j * 128, (j + 1) * 128)
        far = lax.dot_general(query, recv_ref[cols, :], (((1,), (1,)), ((), ())), preferred_element_type=F32)
        gated = near_ref[:, cols] + lift_ref[:, cols] * far
        squares = squares + jnp.sum(gated * gated, axis=1, keepdims=True)
        feat_ref[:, cols] = (gated * gain_ref[:, cols]).astype(BF16)
    square_ref[...] = jnp.broadcast_to(squares, (TOK, 128))
    product_rows(feat_ref, square_ref, ow_ref, first_ref, second_ref, 1 - (lax.axis_index("head") & 1))


def product_rows(feat_ref, square_ref, ow_ref, first_ref, second_ref, side):
    y = lax.axis_index("head") >> 1
    lane = lax.broadcasted_iota(jnp.int32, (32, 128), 1)
    starts = [pl.multiple_of((2 * jnp.bitwise_xor(y, k) + side) * 32, 32) for k in (3, 2, 1, 0)]
    rows = jnp.concatenate([feat_ref[pl.ds(s, 32), :] for s in starts], axis=0)
    product = dot(rows, ow_ref[...]).astype(BF16)
    first_ref[:, 0:DM] = product[0:32]
    second_ref[:, 0:DM] = product[32:128]
    for i, s in enumerate(starts):
        high, low = split_two(square_ref[pl.ds(s, 32), :])
        out_ref, at = (first_ref, 0) if i == 0 else (second_ref, (i - 1) * 32)
        out_ref[at : at + 32, DM:WIDE] = jnp.where(
            lane < 64, high.astype(F32), low.astype(F32)
        ).astype(BF16)


def own_rows_kernel(feat_ref, square_ref, ow_ref, first_ref, second_ref):
    product_rows(feat_ref, square_ref, ow_ref, first_ref, second_ref, lax.axis_index("head") & 1)


def squares_at(ref, rows, at):
    return ref[rows, at : at + 1].astype(F32) + ref[rows, at + 64 : at + 65].astype(F32)


def pair_kernel(mine_ref, recv_ref, *out_refs):
    lane = lax.broadcasted_iota(jnp.int32, (32, 128), 1)
    for i, out_ref in enumerate(out_refs):
        rows = slice(i * 32, (i + 1) * 32)
        total = mine_ref[rows, 0:DM].astype(F32) + recv_ref[rows, 0:DM].astype(F32)
        out_ref[:, 0:DM] = total.astype(out_ref.dtype)
        square = jnp.broadcast_to(squares_at(mine_ref, rows, DM) + squares_at(recv_ref, rows, DM), (32, 128))
        high, low = split_two(square)
        out_ref[:, DM:WIDE] = jnp.where(lane < 64, high.astype(F32), low.astype(F32)).astype(out_ref.dtype)


def final_kernel(own_ref, r1, r2, r3, out_ref):
    every = slice(0, 32)
    square = sum(squares_at(ref, every, DM) for ref in (own_ref, r1, r2, r3))
    scale = lax.rsqrt(square * (1.0 / (H * P_SIZE)) + EPSILON)
    total = own_ref[:, 0:DM].astype(F32)
    for ref in (r1, r2, r3):
        total = total + ref[:, 0:DM].astype(F32)
    out_ref[...] = (total * scale).astype(BF16)


def call(kernel, outs, *args, scratch=(), flops=0, name=None, smem=(), hbm=(), free=()):
    def space(i):
        if i in smem:
            return pltpu.SMEM
        if i in hbm:
            return pltpu.HBM
        return pl.ANY if i in free else pltpu.VMEM

    specs = [pl.BlockSpec(memory_space=space(i)) for i in range(len(args))]
    args = [pltpu.with_memory_space_constraint(a, pltpu.HBM) if i in hbm else a for i, a in enumerate(args)]
    shapes = [jax.ShapeDtypeStruct(shape, dtype) for shape, dtype in outs]
    outputs = pl.pallas_call(
        kernel,
        out_shape=shapes,
        in_specs=specs,
        out_specs=[pl.BlockSpec(memory_space=pltpu.VMEM) for _ in outs],
        scratch_shapes=list(scratch),
        compiler_params=pltpu.CompilerParams(vmem_limit_bytes=48 << 20),
        cost_estimate=pl.CostEstimate(flops=flops, transcendentals=0, bytes_accessed=flops // 100),
        name=name,
    )(*args)
    return outputs


def on_device(token_values, gate_values, state_in, state_out, step_size, log_decay, level_weight, skip_weight, norm_gain, out_weight):
    step = jnp.transpose(step_size)
    decay = jnp.transpose(log_decay)
    weight = jnp.transpose(level_weight, (1, 2, 0))
    pay, state, xt, cum, total = call(
        state_kernel,
        [((PAY, N), BF16), ((WIDTH, N), F32), ((WIDTH, TOK), BF16), ((16, TOK), F32), ((16, 128), F32)],
        token_values, state_in, step, decay, flops=10**8, name="state", hbm=(0, 1, 2, 3),
        scratch=[
            pltpu.VMEM((TOK, WIDTH), BF16), pltpu.VMEM((TOK, N), BF16), pltpu.VMEM((HEADS, TOK), F32),
            pltpu.VMEM((HEADS, TOK), F32), pltpu.SemaphoreType.DMA((4,)),
        ],
    )
    local, qt = call(
        local_kernel,
        [((WIDTH, TOK), F32), ((N, TOK), BF16)],
        xt, cum, skip_weight, state_in, state_out, step, weight,
        flops=5 * 10**9, name="local", smem=(2,), hbm=(3, 4, 5, 6),
        scratch=[
            pltpu.VMEM((TOK, N), BF16), pltpu.VMEM((TOK, N), BF16), pltpu.VMEM((HEADS, TOK), F32),
            pltpu.VMEM((HEADS, 14, TOK), BF16), pltpu.SemaphoreType.DMA((4,)),
        ],
    )
    r3, r2, r1 = [lax.ppermute(pay, "seq", [(d, d ^ k) for d in range(32)]) for k in (3, 2, 1)]
    pay, next_state, pair, state, total, span1, span2 = call(
        quad_kernel,
        [((PAY, N), BF16), ((WIDTH, N), BF16), ((WIDTH, N), BF16), ((WIDTH, N), F32)] + [((16, 128), F32)] * 3,
        local, r3, r2, r1, state, total, flops=10**6, name="quad", free=(0,),
    )
    recvs, spans = [next_state, pair], [jnp.zeros((16, 128), F32), span1, span2]
    recvs.append(lax.ppermute(pay, "seq", [(d, d ^ 4) for d in range(32)]))
    pay, state, total, span = call(
        lambda *refs: combine_kernel(2, *refs),
        [((PAY, N), BF16), ((WIDTH, N), F32), ((16, 128), F32), ((16, 128), F32)],
        state, total, span2, recvs[2], flops=10**6, name="combine",
    )
    spans.append(span)
    recvs.append(lax.ppermute(pay, "seq", [(d, d ^ 12) for d in range(32)]))
    pay, span = call(
        last_combine_kernel, [((WIDTH, N), BF16), ((16, 128), F32)],
        state, total, span, recvs[3], flops=10**6, name="combine",
    )
    spans.append(span)
    recvs.append(lax.ppermute(pay, "seq", [(d, d ^ 28) for d in range(32)]))
    near, lift = call(
        near_kernel, [((TOK, WIDTH), F32)] * 2,
        local, *recvs[:4], *spans, qt, cum, weight, gate_values,
        flops=2 * 10**9, name="near",
    )
    halves = [((32, WIDE), BF16), ((96, WIDE), BF16)]
    *theirs, feat, square = call(
        feature_kernel,
        [*halves, ((TOK, WIDTH), BF16), ((TOK, 128), F32)],
        near, lift, recvs[4], state_out, norm_gain[None, :], out_weight,
        flops=10**9, name="feature",
    )
    mine = call(own_rows_kernel, halves, feat, square, out_weight, flops=10**9, name="own_rows")
    swap = [(g, g ^ 1) for g in range(8)]
    recv = [lax.ppermute(part, "head", swap) for part in theirs]
    one = ((32, WIDE), BF16)
    (send3,) = call(pair_kernel, [one], mine[0], recv[0], flops=10**6, name="pair")
    send2, send1, own = call(pair_kernel, [one, one, ((32, WIDE), F32)], mine[1], recv[1], flops=10**6, name="pair")
    got = [
        lax.ppermute(send, "head", [(g, g ^ (2 * k)) for g in range(8)])
        for k, send in ((3, send3), (2, send2), (1, send1))
    ]
    (out,) = call(final_kernel, [((32, DM), BF16)], own, *got, flops=10**6, name="final")
    return out


def solution(mesh):
    placed = (
        P("seq", "head"),
        P("seq", "head"),
        P("seq", None),
        P("seq", None),
        P("seq", "head"),
        P("seq", "head"),
        P("seq", "head", None),
        P("head"),
        P("head"),
        P("head", None),
    )
    return jax.shard_map(
        on_device, mesh=mesh, in_specs=placed, out_specs=P(("seq", "head"), None), check_vma=False
    )
```
